32 devices in a mesh: gx: 4 (over x, core), gy: 2 (over y), gz: 4 (over z).
Axes of the slice: x: 2, y: 2, z: 4, core: 2. Of those that a mesh axis runs over, the one named last changes fastest.
Arguments:
- velocity: float32 [3, 512, 512], P(None, None, ('gx', 'gy', 'gz')), may hold values from -4 to 4
- inv_density: float32 [512, 512], P(None, ('gx', 'gy', 'gz')), may hold values from 0.25 to 4
- element_place: int32 [512], P(('gx', 'gy', 'gz')), may hold values from 0 to 15, as said below
Outputs:
- advected: float32 [3, 512, 512], P(None, None, ('gx', 'gy', 'gz'))
- pressure: float32 [512, 512], P(None, ('gx', 'gy', 'gz'))
- residual: float32 [512, 512], P(None, ('gx', 'gy', 'gz'))
The draws below stay inside these ranges and needn't reach their ends.
Inputs may be any that keep to these rules, and one draw needn't show every extreme that they name: `element_place`: within each device's 16 consecutive elements every block position appears exactly once.
All inputs are finite; a program needn't handle non-finite values.
Results may differ from the reference program's by a relative error of at most 0.0003.
Values sent between devices are 32-bit elements; how exact they have to be, the bound alone decides.
A program may use at most 64 MiB of HBM per device.

```python
import math
import jax
import jax.numpy as jnp
from jax import lax

PTS = 512
BX = 4
BY = 4
BZ = 1
CG_ITERS = 2
ELEM_DEV = 16
NEL = 512
N_GX = 4
N_GY = 2
N_GZ = 4


def shuffle_block(block_key):
    return jax.random.permutation(block_key, ELEM_DEV)


def draw_element_place(key, part):
    devices = NEL // ELEM_DEV
    device_keys = jax.random.split(jax.random.fold_in(key, 17), devices)
    orders = jax.vmap(shuffle_block)(device_keys)
    return orders.reshape(NEL).astype(jnp.int32)


def block_levels(key, dims, cuts, least, high):
    def one(dim, parts):
        steps = jax.random.uniform(jax.random.fold_in(jax.random.fold_in(key, 6), dim), (parts,), jnp.float32, least / len(cuts), high / len(cuts))
        return jnp.repeat(jnp.exp(steps), dims[dim] // parts).reshape((-1,) + (1,) * (len(dims) - dim - 1))

    factor_of = one(*cuts[0])
    for cut in cuts[1:]:
        factor_of = factor_of * one(*cut)
    return factor_of


def scatter_about(rng, extent, deviation, most, cuts=(), kind=jnp.bfloat16):
    level = block_levels(rng, extent, cuts, -0.22, 0.18) if cuts else 1.0
    values = jax.random.normal(rng, extent, jnp.float32) * deviation * level
    return jnp.minimum(jnp.maximum(values, -most), most).astype(kind)


def setup_inputs(seed: int = 0) -> dict:
    key_of = jax.random.split(jax.random.key(seed), 4)
    velocity = scatter_about(key_of[0], (3, PTS, NEL), 1.0, 4.0, ((2, 32),), jnp.float32)
    inv_density = jnp.clip(jnp.exp(math.log(4.0) - 2.7725887 * jax.random.uniform(key_of[1], (PTS, NEL), jnp.float32) ** block_levels(key_of[1], (PTS, NEL), ((1, 32),), -0.2, 0.2)), 0.25, 4.0)
    element_place = draw_element_place(jax.random.fold_in(key_of[3], 71), 0)
    return dict(velocity=velocity, inv_density=inv_density, element_place=element_place)


time_step = 0.03
mass_shift = 4.0
contractions = ("ij,sjbce->sibce", "ij,sajce->saice", "ij,sabje->sabie")
inner_nodes = (-0.8717401485096066, -0.5917001814331423, -0.2092992179024789, 0.2092992179024789, 0.5917001814331423, 0.8717401485096066)


def legendre_seven(position):
    previous = 1.0
    current_value = position
    for degree_index in range(1, 7):
        following = ((2 * degree_index + 1) * position * current_value - degree_index * previous) / (degree_index + 1)
        previous = current_value
        current_value = following
    return current_value


def tables():
    node_values = [-1.0] + list(inner_nodes) + [1.0]
    poly_values = [legendre_seven(node) for node in node_values]
    weights = [2.0 / (56.0 * value * value) for value in poly_values]
    derivative = [[0.0] * 8 for row_index in range(8)]
    for row_index in range(8):
        for col_index in range(8):
            if row_index != col_index:
                derivative[row_index][col_index] = poly_values[row_index] / (poly_values[col_index] * (node_values[row_index] - node_values[col_index]))
    derivative[0][0] = -14.0
    derivative[7][7] = 14.0
    squared_t = [[derivative[col_index][row_index] ** 2 for col_index in range(8)] for row_index in range(8)]
    quad_list = [weights[first] * weights[second] * weights[third] for first in range(8) for second in range(8) for third in range(8)]
    quadrature = jnp.asarray(quad_list, jnp.float32).reshape(1, 8, 8, 8, 1)
    return (quadrature, jnp.asarray(derivative, jnp.float32), jnp.asarray(squared_t, jnp.float32))


def apply_along(matrix, values, direction):
    return jnp.einsum(contractions[direction], matrix, values, precision=lax.Precision.HIGHEST)


def multiplicity(offsets, totals, block_shape, elements):
    slot_index = jnp.arange(elements, dtype=jnp.int32)
    places = (slot_index // (block_shape[1] * block_shape[2]), slot_index // block_shape[2] % block_shape[1], slot_index % block_shape[2])
    node_index = jnp.arange(8, dtype=jnp.int32)
    first_node = (node_index == 0).astype(jnp.float32)[:, None]
    last_node = (node_index == 7).astype(jnp.float32)[:, None]
    factors = []
    for direction in range(3):
        position = places[direction] + offsets[direction]
        lower_open = (position > 0).astype(jnp.float32)[None, :]
        upper_open = (position < totals[direction] - 1).astype(jnp.float32)[None, :]
        factors.append(1.0 + first_node * lower_open + last_node * upper_open)
    joined = factors[0][:, None, None, :] * factors[1][None, :, None, :] * factors[2][None, None, :, :]
    return joined[None]


def assemble_axis(values, point_axis, grid_axis, block_shape, sender):
    lower_faces = lax.index_in_dim(values, 0, point_axis, keepdims=False)
    upper_faces = lax.index_in_dim(values, 7, point_axis, keepdims=False)
    flat_shape = lower_faces.shape
    grid_shape = flat_shape[:3] + tuple(block_shape)
    lower_faces = lower_faces.reshape(grid_shape)
    upper_faces = upper_faces.reshape(grid_shape)
    element_axis = 3 + grid_axis
    length = block_shape[grid_axis]
    interior = lax.slice_in_dim(upper_faces, 0, length - 1, axis=element_axis) + lax.slice_in_dim(lower_faces, 1, length, axis=element_axis)
    lower_edge = lax.slice_in_dim(lower_faces, 0, 1, axis=element_axis)
    upper_edge = lax.slice_in_dim(upper_faces, length - 1, length, axis=element_axis)
    arrived = sender(jnp.stack([lower_edge, upper_edge]))
    first_sum = lower_edge + arrived[0]
    last_sum = upper_edge + arrived[3]
    new_lower = jnp.concatenate([first_sum, interior], axis=element_axis).reshape(flat_shape)
    new_upper = jnp.concatenate([interior, last_sum], axis=element_axis).reshape(flat_shape)
    values = lax.dynamic_update_slice_in_dim(values, jnp.expand_dims(new_lower, point_axis), 0, point_axis)
    values = lax.dynamic_update_slice_in_dim(values, jnp.expand_dims(new_upper, point_axis), 7, point_axis)
    return values


def pad_sender(face_pair):
    return jnp.pad(face_pair, [(1, 1)] + [(0, 0)] * (face_pair.ndim - 1))


def invert_order(ordering):
    return jnp.zeros((ordering.shape[0],), jnp.int32).at[ordering].set(jnp.arange(ordering.shape[0], dtype=jnp.int32))


def to_grid(array, inverse, devices):
    leading = array.shape[:-1]
    rank_lead = len(leading)
    blocks = array.reshape(leading + (devices, ELEM_DEV))
    index_full = jnp.broadcast_to(inverse.reshape((1,) * rank_lead + (devices, ELEM_DEV)), blocks.shape)
    blocks = jnp.take_along_axis(blocks, index_full, axis=-1)
    blocks = blocks.reshape(leading + (N_GX, N_GY, N_GZ, BX, BY, BZ))
    axes_order = list(range(rank_lead)) + [rank_lead + 0, rank_lead + 3, rank_lead + 1, rank_lead + 4, rank_lead + 2, rank_lead + 5]
    return blocks.transpose(axes_order).reshape(leading + (-1,))


def from_grid(array, orders, devices):
    leading = array.shape[:-1]
    rank_lead = len(leading)
    blocks = array.reshape(leading + (N_GX, BX, N_GY, BY, N_GZ, BZ))
    axes_order = list(range(rank_lead)) + [rank_lead + 0, rank_lead + 2, rank_lead + 4, rank_lead + 1, rank_lead + 3, rank_lead + 5]
    blocks = blocks.transpose(axes_order).reshape(leading + (devices, ELEM_DEV))
    index_full = jnp.broadcast_to(orders.reshape((1,) * rank_lead + (devices, ELEM_DEV)), blocks.shape)
    return jnp.take_along_axis(blocks, index_full, axis=-1).reshape(leading + (-1,))


def reference(velocity, inv_density, element_place):
    devices = N_GX * N_GY * N_GZ
    grid_shape = (BX * N_GX, BY * N_GY, BZ * N_GZ)
    orders = element_place.reshape(devices, ELEM_DEV)
    inverse = jax.vmap(invert_order)(orders)
    quadrature, derivative, square_table = tables()
    advector = to_grid(velocity, inverse, devices).reshape(3, 8, 8, 8, -1)
    mobility = to_grid(inv_density, inverse, devices).reshape(1, 8, 8, 8, -1)
    elements = advector.shape[-1]
    copies = multiplicity((0, 0, 0), grid_shape, grid_shape, elements)
    mass = quadrature * copies
    inverse_copies = 1.0 / copies

    def assemble(values):
        values = assemble_axis(values, 1, 0, grid_shape, pad_sender)
        values = assemble_axis(values, 2, 1, grid_shape, pad_sender)
        return assemble_axis(values, 3, 2, grid_shape, pad_sender)

    def advection_rate(section_value):
        convective = advector[0:1] * apply_along(derivative, section_value, 0)
        convective = convective + advector[1:2] * apply_along(derivative, section_value, 1)
        convective = convective + advector[2:3] * apply_along(derivative, section_value, 2)
        return assemble(-quadrature * convective) / mass

    first_rate = advection_rate(advector)
    second_rate = advection_rate(advector + 0.5 * time_step * first_rate)
    third_rate = advection_rate(advector + 0.5 * time_step * second_rate)
    fourth_rate = advection_rate(advector + time_step * third_rate)
    advected = advector + (time_step / 6.0) * (first_rate + 2.0 * second_rate + 2.0 * third_rate + fourth_rate)

    divergence = apply_along(derivative, advected[0:1], 0) + apply_along(derivative, advected[1:2], 1) + apply_along(derivative, advected[2:3], 2)
    weighted = quadrature * mobility
    diag_local = mass_shift * quadrature + apply_along(square_table, weighted, 0) + apply_along(square_table, weighted, 1) + apply_along(square_table, weighted, 2)
    source_local = -quadrature * divergence / time_step
    assembled = assemble(jnp.concatenate([source_local, diag_local], axis=0))
    source = assembled[0:1]
    inverse_jacobi = 1.0 / assembled[1:2]

    def operator(values):
        summed = mass_shift * quadrature * values
        for direction in range(3):
            slope = apply_along(derivative, values, direction)
            summed = summed + apply_along(derivative.T, weighted * slope, direction)
        return assemble(summed)

    def inner(left, right):
        return jnp.sum(left * right * inverse_copies)

    pressure = jnp.zeros_like(source)
    residual = source
    precond = residual * inverse_jacobi
    search = precond
    current = inner(residual, precond)
    for iteration in range(CG_ITERS):
        applied = operator(search)
        step_size = current / inner(search, applied)
        pressure = pressure + step_size * search
        residual = residual - step_size * applied
        if iteration + 1 < CG_ITERS:
            precond = residual * inverse_jacobi
            following = inner(residual, precond)
            search = precond + (following / current) * search
            current = following
    advected_out = from_grid(advected.reshape(3, 512, -1), orders, devices)
    pressure_out = from_grid(pressure.reshape(512, -1), orders, devices)
    residual_out = from_grid(residual.reshape(512, -1), orders, devices)
    return advected_out, pressure_out, residual_out
```

```python
import functools

import jax
import jax.numpy as jnp
import numpy as np
from jax import lax
from jax.experimental import pallas as pl
from jax.experimental.pallas import tpu as pltpu
from jax.sharding import PartitionSpec as P

BX = 4
BY = 4
BZ = 1
MESH = pl.DeviceIdType.MESH
AXES = ("gx", "gy", "gz")
ROUNDS = 7

time_step = 0.03
mass_shift = 4.0
inner_nodes = (
    -0.8717401485096066,
    -0.5917001814331423,
    -0.2092992179024789,
    0.2092992179024789,
    0.5917001814331423,
    0.8717401485096066,
)


def legendre_seven(position):
    previous = 1.0
    current_value = position
    for degree_index in range(1, 7):
        following = (
            (2 * degree_index + 1) * position * current_value - degree_index * previous
        ) / (degree_index + 1)
        previous = current_value
        current_value = following
    return current_value


def tables():
    nodes = [-1.0] + list(inner_nodes) + [1.0]
    poly = [legendre_seven(node) for node in nodes]
    weights = np.array([2.0 / (56.0 * value * value) for value in poly])
    derivative = np.zeros((8, 8))
    for i in range(8):
        for j in range(8):
            if i != j:
                derivative[i, j] = poly[i] / (poly[j] * (nodes[i] - nodes[j]))
    derivative[0, 0] = -14.0
    derivative[7, 7] = 14.0
    return weights, derivative.astype(np.float32).astype(np.float64)


def lane_rows(matrix):
    rows = np.zeros((32, 128))
    for t in range(4):
        for u in range(4):
            for h in range(2):
                rows[8 * t + 2 * u, 64 * h : 64 * h + 64] = matrix[2 * t + h, 2 * u + h]
                rows[8 * t + 2 * u + 1, 64 * h : 64 * h + 64] = matrix[2 * t + h, 2 * u + 1 - h]
    return rows


def split_stack(matrix):
    wide = jnp.asarray(matrix, jnp.float32)
    high = np.asarray(matrix, np.float32).astype(jnp.bfloat16)
    low = (np.asarray(matrix, np.float32) - high.astype(np.float32)).astype(jnp.bfloat16)
    del wide
    return np.concatenate([high, high, low], axis=0)


@functools.cache
def constants():
    weights, d = tables()
    eye2, eye8, eye16 = np.eye(2), np.eye(8), np.eye(16)
    forward = np.concatenate(
        [np.kron(np.kron(eye2, d.T), eye8), np.kron(eye16, d.T)], axis=1
    )
    backward = np.concatenate([np.kron(np.kron(eye2, d), eye8), np.kron(eye16, d)], axis=0)
    square = np.kron(np.kron(eye2, d**2), eye8) + np.kron(eye16, d**2)
    quad = np.einsum("a,b,c->abc", weights, weights, weights).reshape(4, 128)
    rows = np.concatenate(
        [lane_rows(d), lane_rows(d.T), lane_rows(d.T**2), quad, np.zeros((4, 128))], axis=0
    )
    return (
        rows.astype(np.float32),
        split_stack(forward),
        split_stack(backward),
        split_stack(square),
    )


def kernel(
    counts,
    vel_ref,
    den_ref,
    place_ref,
    rows_ref,
    fwd_ref,
    bwd_ref,
    sqr_ref,
    adv_ref,
    pre_ref,
    res_ref,
    send_x,
    send_y,
    send_z,
    recv_x,
    recv_y,
    recv_z,
    sums,
    sums_x,
    sums_y,
    sums_z,
    send_sem,
    recv_sem,
    sum_send,
    sum_recv,
):
    f32 = jnp.float32
    me = [lax.axis_index(name) for name in AXES]
    sends = (send_x, send_y, send_z)
    recvs = (recv_x, recv_y, recv_z)
    has = [(me[i] > 0, me[i] < counts[i] - 1) for i in range(3)]

    def at(axis, position):
        return tuple(position if i == axis else me[i] for i in range(3))

    for axis in range(3):
        for side in range(2):

            @pl.when(jnp.logical_not(has[axis][side]))
            def _():
                for r in range(ROUNDS):
                    recvs[axis][r, side] = jnp.zeros(recvs[axis].shape[2:], f32)

    barrier = pltpu.get_barrier_semaphore()
    greeted = 0
    for axis in range(3):
        for k in range(1, counts[axis]):
            pl.semaphore_signal(
                barrier,
                inc=1,
                device_id=at(axis, lax.rem(me[axis] + k, counts[axis])),
                device_id_type=MESH,
            )
            greeted += 1

    lane = lax.broadcasted_iota(jnp.int32, (1, 16, 128), 2)
    row = lax.broadcasted_iota(jnp.int32, (1, 16, 128), 1)
    ex, ey = row // BY, row % BY
    node_b, node_c = (lane // 8) % 8, lane % 8

    r16 = lax.broadcasted_iota(jnp.int32, (16, 16), 0)
    l16 = lax.broadcasted_iota(jnp.int32, (16, 16), 1)
    by_lane = jnp.zeros((16, 16), jnp.int32)
    by_row = jnp.zeros((16, 16), jnp.int32)
    for e in range(16):
        by_lane = jnp.where(l16 == e, place_ref[e], by_lane)
        by_row = jnp.where(r16 == e, place_ref[e], by_row)
    to_place = (by_lane == r16).astype(f32)
    to_slot = (by_row == l16).astype(f32)

    def order(matrix, block):
        return jnp.dot(
            matrix, block, precision=lax.Precision.HIGHEST, preferred_element_type=f32
        )

    placed = [order(to_place, vel_ref[i]) for i in range(3)]
    velocity = [
        jnp.stack([placed[i][:, 128 * t : 128 * t + 128] for i in range(3)]) for t in range(4)
    ]
    dens = order(to_place, den_ref[...])
    quad = [rows_ref[96 + t : 97 + t, :].reshape(1, 1, 128) for t in range(4)]
    mobile = [quad[t] * dens[:, 128 * t : 128 * t + 128].reshape(1, 16, 128) for t in range(4)]

    def half(flag):
        return jnp.where(flag, 0.5, 1.0).astype(f32)

    total = [BX * counts[0], BY * counts[1], BZ * counts[2]]
    pos_x, pos_y = ex + me[0] * BX, ey + me[1] * BY
    share_y = half(
        ((node_b == 0) & (pos_y > 0)) | ((node_b == 7) & (pos_y < total[1] - 1))
    )
    pos_z = row * 0 + me[2]
    share_z = half(((node_c == 0) & (pos_z > 0)) | ((node_c == 7) & (pos_z < total[2] - 1)))
    share_yz = share_y * share_z
    share = [share_yz] * 4
    share[0] = share_yz * half((lane < 64) & (pos_x > 0))
    share[3] = share_yz * half((lane >= 64) & (pos_x < total[0] - 1))

    def along_x(base, v):
        swapped = [pltpu.roll(v[t], 64, 2) for t in range(4)]
        out = []
        for t in range(4):
            acc = None
            for u in range(4):
                k = base + 8 * t + 2 * u
                term = (
                    rows_ref[k : k + 1, :].reshape(1, 1, 128) * v[u]
                    + rows_ref[k + 1 : k + 2, :].reshape(1, 1, 128) * swapped[u]
                )
                acc = term if acc is None else acc + term
            out.append(acc)
        return out

    def split(x):
        high = x.astype(jnp.bfloat16)
        low = (x - high.astype(f32)).astype(jnp.bfloat16)
        return jnp.concatenate([high, low, high], axis=1)

    def along_lanes(v, w_ref):
        c = v[0].shape[0]
        x = jnp.concatenate([v[t].reshape(c * 16, -1) for t in range(4)], axis=0)
        y = jnp.dot(split(x), w_ref[...], preferred_element_type=f32)
        return [y[t * c * 16 : (t + 1) * c * 16].reshape(c, 16, -1) for t in range(4)]

    def copy(r, axis, side, c):
        peer = me[axis] + (1 if side else -1)
        return pltpu.make_async_remote_copy(
            src_ref=sends[axis].at[r, side, pl.ds(0, c)],
            dst_ref=recvs[axis].at[r, 1 - side, pl.ds(0, c)],
            send_sem=send_sem.at[r, axis, side],
            recv_sem=recv_sem.at[r, axis, 1 - side],
            device_id=at(axis, peer),
            device_id_type=MESH,
        )

    def arrival(r, axis, side, c):
        peer = me[axis] + (1 if side else -1)
        return pltpu.make_async_remote_copy(
            src_ref=sends[axis].at[r, side, pl.ds(0, c)],
            dst_ref=recvs[axis].at[r, side, pl.ds(0, c)],
            send_sem=send_sem.at[r, axis, side],
            recv_sem=recv_sem.at[r, axis, side],
            device_id=at(axis, peer),
            device_id_type=MESH,
        )

    def start(r, axis, c):
        for side in range(2):

            @pl.when(has[axis][side])
            def _():
                copy(r, axis, side, c).start()

    def finish(r, axis, c):
        for side in range(2):

            @pl.when(has[axis][side])
            def _():
                arrival(r, axis, side, c).wait_recv()

    def nothing(axis):
        return None

    def assemble(v, r, before=nothing, after=nothing):
        v = list(v)
        c = v[0].shape[0]
        lower, upper = pltpu.roll(v[0], 64, 2), pltpu.roll(v[3], 64, 2)
        send_x[r, 0, :c] = lower[:, 0:8]
        send_x[r, 1, :c] = upper[:, 8:16]
        start(r, 0, c)
        before(0)
        finish(r, 0, c)
        after(0)
        from_low = jnp.concatenate([upper[:, 0:8], recv_x[r, 0, :c]], axis=1)
        from_high = jnp.concatenate([recv_x[r, 1, :c], lower[:, 8:16]], axis=1)
        d_low = pltpu.roll(jnp.where(row < 12, upper, from_low), 4, 1)
        d_high = pltpu.roll(jnp.where(row >= 4, lower, from_high), 12, 1)
        v[0] = v[0] + jnp.where(lane < 64, d_low, 0.0)
        v[3] = v[3] + jnp.where(lane >= 64, d_high, 0.0)
        lower = v[0]
        upper = pltpu.roll(v[0], 72, 2)
        for t in range(1, 4):
            lower = jnp.where(node_b == t, pltpu.roll(v[t], 8 * t, 2), lower)
            upper = jnp.where(node_b == t, pltpu.roll(v[t], 72 + 8 * t, 2), upper)
        send_y[r, 0, :c] = lower
        send_y[r, 1, :c] = upper
        start(r, 1, c)
        before(1)
        in_low, in_high = pltpu.roll(upper, 1, 1), pltpu.roll(lower, 15, 1)
        finish(r, 1, c)
        after(1)
        d_low = jnp.where(ey > 0, in_low, pltpu.roll(recv_y[r, 0, :c], 13, 1))
        d_high = jnp.where(ey < 3, in_high, pltpu.roll(recv_y[r, 1, :c], 3, 1))
        for t in range(4):
            low = d_low if t == 0 else pltpu.roll(d_low, 128 - 8 * t, 2)
            high = pltpu.roll(d_high, 56 - 8 * t, 2)
            v[t] = v[t] + jnp.where(node_b == 0, low, jnp.where(node_b == 7, high, 0.0))
        lower = v[0]
        upper = pltpu.roll(v[0], 121, 2)
        for t in range(1, 4):
            lower = jnp.where(node_c == t, pltpu.roll(v[t], t, 2), lower)
            upper = jnp.where(node_c == t, pltpu.roll(v[t], 121 + t, 2), upper)
        send_z[r, 0, :c] = lower
        send_z[r, 1, :c] = upper
        start(r, 2, c)
        before(2)
        finish(r, 2, c)
        after(2)
        d_low, d_high = recv_z[r, 0, :c], recv_z[r, 1, :c]
        for t in range(4):
            low = d_low if t == 0 else pltpu.roll(d_low, 128 - t, 2)
            high = pltpu.roll(d_high, 7 - t, 2)
            v[t] = v[t] + jnp.where(node_c == 0, low, jnp.where(node_c == 7, high, 0.0))
        return v

    def advect(v):
        dx = along_x(0, v)
        dyz = along_lanes(v, fwd_ref)
        return [
            velocity[t][0:1] * dx[t]
            + velocity[t][1:2] * dyz[t][:, :, :128]
            + velocity[t][2:3] * dyz[t][:, :, 128:]
            for t in range(4)
        ]

    first = advect(velocity)
    square_x = along_x(64, mobile)
    square_yz = along_lanes(mobile, sqr_ref)
    diag = [mass_shift * quad[t] + square_x[t] + square_yz[t] for t in range(4)]
    pl.semaphore_wait(barrier, greeted)
    joint = assemble([jnp.concatenate([first[t], diag[t]], axis=0) for t in range(4)], 0)
    inverse_jacobi = [1.0 / joint[t][3:4] for t in range(4)]
    k1 = [joint[t][0:3] * share[t] for t in range(4)]
    total_rate = k1
    v = [velocity[t] - (0.5 * time_step) * k1[t] for t in range(4)]
    for r, step, weight in ((1, 0.5, 2.0), (2, 1.0, 2.0), (3, 0.0, 1.0)):
        g = assemble(advect(v), r)
        g = [g[t] * share[t] for t in range(4)]
        total_rate = [total_rate[t] + weight * g[t] for t in range(4)]
        if step:
            v = [velocity[t] - (step * time_step) * g[t] for t in range(4)]
    advected = [velocity[t] - (time_step / 6.0) * total_rate[t] for t in range(4)]

    dx = along_x(0, [advected[t][0:1] for t in range(4)])
    dyz = along_lanes([advected[t][1:3] for t in range(4)], fwd_ref)
    div = [dx[t] + dyz[t][0:1, :, :128] + dyz[t][1:2, :, 128:] for t in range(4)]
    source = assemble(div, 4)
    r0 = [source[t] * (quad[t] * (-1.0 / time_step)) for t in range(4)]

    def local(v):
        dx = along_x(0, v)
        dyz = along_lanes(v, fwd_ref)
        gx = [mobile[t] * dx[t] for t in range(4)]
        gyz = [
            jnp.concatenate(
                [mobile[t] * dyz[t][:, :, :128], mobile[t] * dyz[t][:, :, 128:]], axis=2
            )
            for t in range(4)
        ]
        bx = along_x(32, gx)
        byz = along_lanes(gyz, bwd_ref)
        return [(mass_shift * quad[t]) * v[t] + bx[t] + byz[t] for t in range(4)]

    def dot_row(a, b, scale=None):
        acc = None
        for t in range(4):
            term = a[t] * b[t]
            if scale is not None:
                term = term * scale[t]
            acc = term if acc is None else acc + term
        return jnp.sum(acc[0], axis=0, keepdims=True)

    z0 = [r0[t] * inverse_jacobi[t] for t in range(4)]
    lz = local(z0)
    rho_row = dot_row(r0, z0, share)
    gamma_row = dot_row(z0, lz)
    s = assemble(lz, 5)
    w = [s[t] * inverse_jacobi[t] for t in range(4)]
    lw = local(w)
    delta_row = dot_row(s, w, share)
    eps_row = dot_row(w, lw)
    sums[0] = jnp.concatenate(
        [rho_row, gamma_row, delta_row, eps_row, jnp.zeros((4, 128), f32)], axis=0
    )
    sum_bufs = (sums_x, sums_y, sums_z)

    def sum_copy(axis, k):
        return pltpu.make_async_remote_copy(
            src_ref=sums.at[axis],
            dst_ref=sum_bufs[axis].at[k - 1],
            send_sem=sum_send[axis].at[k - 1],
            recv_sem=sum_recv[axis].at[k - 1],
            device_id=at(axis, lax.rem(me[axis] + k, counts[axis])),
            device_id_type=MESH,
        )

    def sum_start(axis):
        for k in range(1, counts[axis]):
            sum_copy(axis, k).start()

    def sum_finish(axis):
        joined = sums[axis]
        for k in range(1, counts[axis]):
            sum_copy(axis, k).wait_recv()
            joined = joined + sum_bufs[axis][k - 1]
        sums[axis + 1] = joined

    t_vec = assemble(lw, 6, sum_start, sum_finish)
    four = jnp.sum(sums[3], axis=1, keepdims=True)
    rho, gamma, delta, eps = (four[i : i + 1].reshape(1, 1, 1) for i in range(4))
    alpha0 = rho / gamma
    rho1 = rho - 2.0 * alpha0 * gamma + alpha0 * alpha0 * delta
    beta = rho1 / rho
    cross = gamma - alpha0 * delta
    curve = gamma - 2.0 * alpha0 * delta + alpha0 * alpha0 * eps
    curve = curve + 2.0 * beta * cross + beta * beta * gamma
    alpha1 = rho1 / curve
    along = alpha0 + alpha1 * (1.0 + beta)
    side_step = alpha0 * alpha1

    def put(field):
        return order(to_slot, field)

    for i in range(3):
        adv_ref[i] = put(jnp.concatenate([advected[t][i] for t in range(4)], axis=1))
    pre_ref[...] = put(
        jnp.concatenate([(along * z0[t] - side_step * w[t])[0] for t in range(4)], axis=1)
    )
    res_ref[...] = put(
        jnp.concatenate(
            [(r0[t] - along * s[t] + side_step * t_vec[t])[0] for t in range(4)], axis=1
        )
    )
    for r in range(ROUNDS):
        c = 4 if r == 0 else 3 if r < 4 else 1
        for axis in range(3):
            for side in range(2):

                @pl.when(has[axis][side])
                def _():
                    copy(r, axis, side, c).wait_send()

    for axis in range(3):
        for k in range(1, counts[axis]):
            sum_copy(axis, k).wait_send()


def per_device(counts, velocity, inv_density, element_place):
    f32 = jnp.float32
    rows, forward, backward, square = constants()
    elements = element_place.shape[0]
    points = inv_density.shape[0]
    vmem = pl.BlockSpec(memory_space=pltpu.VMEM)
    faces_x = pltpu.VMEM((ROUNDS, 2, 4, 8, 128), f32)
    faces = pltpu.VMEM((ROUNDS, 2, 4, 16, 128), f32)
    dma = pltpu.SemaphoreType.DMA
    peers = [n - 1 for n in counts]
    advected, pressure, residual = pl.pallas_call(
        functools.partial(kernel, counts),
        out_shape=(
            jax.ShapeDtypeStruct((3, elements, points), f32),
            jax.ShapeDtypeStruct((elements, points), f32),
            jax.ShapeDtypeStruct((elements, points), f32),
        ),
        in_specs=[vmem, vmem, pl.BlockSpec(memory_space=pltpu.SMEM), vmem, vmem, vmem, vmem],
        out_specs=(vmem, vmem, vmem),
        scratch_shapes=[
            faces_x,
            faces,
            faces,
            faces_x,
            faces,
            faces,
            pltpu.VMEM((4, 8, 128), f32),
            pltpu.VMEM((peers[0], 8, 128), f32),
            pltpu.VMEM((peers[1], 8, 128), f32),
            pltpu.VMEM((peers[2], 8, 128), f32),
            dma((ROUNDS, 3, 2)),
            dma((ROUNDS, 3, 2)),
            [dma((n,)) for n in peers],
            [dma((n,)) for n in peers],
        ],
        compiler_params=pltpu.CompilerParams(collective_id=0, has_side_effects=True),
    )(
        velocity.transpose(0, 2, 1),
        inv_density.T,
        element_place,
        jnp.asarray(rows),
        jnp.asarray(forward),
        jnp.asarray(backward),
        jnp.asarray(square),
    )
    return advected.transpose(0, 2, 1), pressure.T, residual.T


def solution(mesh):
    counts = tuple(mesh.shape[name] for name in AXES)
    placed = (P(None, None, AXES), P(None, AXES), P(AXES))
    return jax.shard_map(
        functools.partial(per_device, counts),
        mesh=mesh,
        in_specs=placed,
        out_specs=(P(None, None, AXES), P(None, AXES), P(None, AXES)),
        check_vma=False,
    )
```

```python
import functools

import jax
import jax.numpy as jnp
import numpy as np
from jax import lax
from jax.experimental import pallas as pl
from jax.experimental.pallas import tpu as pltpu
from jax.sharding import PartitionSpec as P

BX = 4
BY = 4
BZ = 1
MESH = pl.DeviceIdType.MESH
AXES = ("gx", "gy", "gz")
ROUNDS = 7

time_step = 0.03
mass_shift = 4.0
inner_nodes = (
    -0.8717401485096066,
    -0.5917001814331423,
    -0.2092992179024789,
    0.2092992179024789,
    0.5917001814331423,
    0.8717401485096066,
)


def legendre_seven(position):
    previous = 1.0
    current_value = position
    for degree_index in range(1, 7):
        following = (
            (2 * degree_index + 1) * position * current_value - degree_index * previous
        ) / (degree_index + 1)
        previous = current_value
        current_value = following
    return current_value


def tables():
    nodes = [-1.0] + list(inner_nodes) + [1.0]
    poly = [legendre_seven(node) for node in nodes]
    weights = np.array([2.0 / (56.0 * value * value) for value in poly])
    derivative = np.zeros((8, 8))
    for i in range(8):
        for j in range(8):
            if i != j:
                derivative[i, j] = poly[i] / (poly[j] * (nodes[i] - nodes[j]))
    derivative[0, 0] = -14.0
    derivative[7, 7] = 14.0
    return weights, derivative.astype(np.float32).astype(np.float64)


def lane_rows(matrix):
    rows = np.zeros((32, 128))
    for t in range(4):
        for u in range(4):
            for h in range(2):
                rows[8 * t + 2 * u, 64 * h : 64 * h + 64] = matrix[2 * t + h, 2 * u + h]
                rows[8 * t + 2 * u + 1, 64 * h : 64 * h + 64] = matrix[2 * t + h, 2 * u + 1 - h]
    return rows


def split_stack(matrix):
    high = np.asarray(matrix, np.float32).astype(jnp.bfloat16)
    low = (np.asarray(matrix, np.float32) - high.astype(np.float32)).astype(jnp.bfloat16)
    return np.concatenate([high, high, low], axis=0)


@functools.cache
def constants():
    weights, d = tables()
    eye2, eye8, eye16 = np.eye(2), np.eye(8), np.eye(16)
    forward = np.concatenate(
        [np.kron(np.kron(eye2, d.T), eye8), np.kron(eye16, d.T)], axis=1
    )
    backward = np.concatenate([np.kron(np.kron(eye2, d), eye8), np.kron(eye16, d)], axis=0)
    square = np.kron(np.kron(eye2, d**2), eye8) + np.kron(eye16, d**2)
    quad = np.einsum("a,b,c->abc", weights, weights, weights).reshape(4, 128)
    rows = np.concatenate(
        [lane_rows(d), lane_rows(d.T), lane_rows(d.T**2), quad, np.zeros((4, 128))], axis=0
    )
    return (
        rows.astype(np.float32),
        split_stack(forward),
        split_stack(backward),
        split_stack(square),
    )


def kernel(
    counts,
    vel_ref,
    den_ref,
    place_ref,
    rows_ref,
    fwd_ref,
    bwd_ref,
    sqr_ref,
    adv_ref,
    pre_ref,
    res_ref,
    send_x,
    send_y,
    send_z,
    recv_xy,
    recv_z,
    sums,
    sums_x,
    sums_y,
    sums_z,
    send_sem,
    recv_sem,
    sum_send,
    sum_recv,
):
    f32 = jnp.float32
    me = [lax.axis_index(name) for name in AXES]
    has = [(me[i] > 0, me[i] < counts[i] - 1) for i in range(3)]

    def at(axis, position):
        return tuple(position if i == axis else me[i] for i in range(3))

    lane = lax.broadcasted_iota(jnp.int32, (1, 16, 128), 2)
    row = lax.broadcasted_iota(jnp.int32, (1, 16, 128), 1)
    ex, ey = row // BY, row % BY
    node_b, node_c = (lane // 8) % 8, lane % 8

    r16 = lax.broadcasted_iota(jnp.int32, (16, 16), 0)
    l16 = lax.broadcasted_iota(jnp.int32, (16, 16), 1)
    by_lane = jnp.zeros((16, 16), jnp.int32)
    by_row = jnp.zeros((16, 16), jnp.int32)
    for e in range(16):
        by_lane = jnp.where(l16 == e, place_ref[e], by_lane)
        by_row = jnp.where(r16 == e, place_ref[e], by_row)
    to_place = (by_lane == r16).astype(f32)
    to_slot = (by_row == l16).astype(f32)

    def order(matrix, block):
        return jnp.dot(
            matrix, block, precision=lax.Precision.HIGHEST, preferred_element_type=f32
        )

    placed = [order(to_place, vel_ref[i]) for i in range(3)]
    velocity = [
        jnp.stack([placed[i][:, 128 * t : 128 * t + 128] for i in range(3)]) for t in range(4)
    ]
    dens = order(to_place, den_ref[...])
    quad = [rows_ref[96 + t : 97 + t, :].reshape(1, 1, 128) for t in range(4)]
    mobile = [quad[t] * dens[:, 128 * t : 128 * t + 128].reshape(1, 16, 128) for t in range(4)]

    def half(flag):
        return jnp.where(flag, 0.5, 1.0).astype(f32)

    total = [BX * counts[0], BY * counts[1], BZ * counts[2]]
    pos_x, pos_y = ex + me[0] * BX, ey + me[1] * BY
    share_y = half(
        ((node_b == 0) & (pos_y > 0)) | ((node_b == 7) & (pos_y < total[1] - 1))
    )
    pos_z = row * 0 + me[2]
    share_z = half(((node_c == 0) & (pos_z > 0)) | ((node_c == 7) & (pos_z < total[2] - 1)))
    share_yz = share_y * share_z
    share = [share_yz] * 4
    share[0] = share_yz * half((lane < 64) & (pos_x > 0))
    share[3] = share_yz * half((lane >= 64) & (pos_x < total[0] - 1))

    def along_x(base, v):
        swapped = [pltpu.roll(v[t], 64, 2) for t in range(4)]
        out = []
        for t in range(4):
            acc = None
            for u in range(4):
                k = base + 8 * t + 2 * u
                term = (
                    rows_ref[k : k + 1, :].reshape(1, 1, 128) * v[u]
                    + rows_ref[k + 1 : k + 2, :].reshape(1, 1, 128) * swapped[u]
                )
                acc = term if acc is None else acc + term
            out.append(acc)
        return out

    def split(x):
        high = x.astype(jnp.bfloat16)
        low = (x - high.astype(f32)).astype(jnp.bfloat16)
        return jnp.concatenate([high, low, high], axis=1)

    def along_lanes(v, w_ref):
        c = v[0].shape[0]
        x = jnp.concatenate([v[t].reshape(c * 16, -1) for t in range(4)], axis=0)
        y = jnp.dot(split(x), w_ref[...], preferred_element_type=f32)
        return [y[t * c * 16 : (t + 1) * c * 16].reshape(c, 16, -1) for t in range(4)]

    directions = [
        (dx, dy, dz)
        for dx in (-1, 1, 0)
        for dy in (0, -1, 1)
        for dz in (0, -1, 1)
        if (dx, dy, dz) != (0, 0, 0)
    ]

    def code(d):
        return (d[0] + 1) * 9 + (d[1] + 1) * 3 + d[2] + 1

    def exists(d):
        flag = None
        for i in range(3):
            if d[i]:
                here = has[i][1 if d[i] > 0 else 0]
                flag = here if flag is None else jnp.logical_and(flag, here)
        return flag

    def side_of(step):
        return 1 if step > 0 else 0

    def source(r, d, c):
        if d[0]:
            return send_x.at[r, side_of(d[0])]
        if d[1]:
            return send_y.at[r, side_of(d[1])]
        return send_z.at[r, side_of(d[2]), pl.ds(0, c)]

    def target(r, d, c):
        if d[0] or d[1]:
            return recv_xy.at[r, code(d)]
        return recv_z.at[r, side_of(d[2]), pl.ds(0, c)]

    def copy(r, d, c, incoming):
        back = d if incoming else tuple(-i for i in d)
        return pltpu.make_async_remote_copy(
            src_ref=source(r, d, c),
            dst_ref=target(r, back, c),
            send_sem=send_sem.at[r, code(d)],
            recv_sem=recv_sem.at[r, code(back)],
            device_id=tuple(me[i] + d[i] for i in range(3)),
            device_id_type=MESH,
        )

    def start(r, c, chosen):
        for d in chosen:

            @pl.when(exists(d))
            def _():
                copy(r, d, c, False).start()

    def finish(r, c):
        for d in directions:

            @pl.when(exists(d))
            def _():
                copy(r, d, c, True).wait_recv()

    barrier = pltpu.get_barrier_semaphore()
    for d in directions:

        @pl.when(exists(d))
        def _():
            pl.semaphore_signal(
                barrier,
                inc=1,
                device_id=tuple(me[i] + d[i] for i in range(3)),
                device_id_type=MESH,
            )

    for axis in range(3):
        for k in range(1, counts[axis]):
            pl.semaphore_signal(
                barrier,
                inc=1,
                device_id=at(axis, lax.rem(me[axis] + k, counts[axis])),
                device_id_type=MESH,
            )
    near = [1 + (me[i] > 0).astype(jnp.int32) + (me[i] < counts[i] - 1).astype(jnp.int32) for i in range(3)]
    greeted = near[0] * near[1] * near[2] - 1 + sum(n - 1 for n in counts)
    for d in directions:

        @pl.when(jnp.logical_not(exists(d)))
        def _():
            for r in range(ROUNDS):
                if d[0] or d[1]:
                    recv_xy[r, code(d)] = jnp.zeros((8, 128), f32)
                else:
                    recv_z[r, side_of(d[2])] = jnp.zeros((4, 8, 128), f32)

    sub8 = lax.broadcasted_iota(jnp.int32, (8, 128), 0)
    lane8 = lax.broadcasted_iota(jnp.int32, (8, 128), 1)
    quarter = sub8 // 4 + 2 * (lane8 // 64)
    b8, c8, y8 = (lane8 // 8) % 8, lane8 % 8, sub8 % 4

    def turn(x, shift, axis):
        size = x.shape[axis]
        shift = shift % size
        return pltpu.roll(x, shift, axis) if shift else x

    def requarter(x, k, base):
        if (k ^ base) & 1:
            x = turn(x, 4, 0)
        if (k ^ base) & 2:
            x = turn(x, 64, 1)
        return x

    def nothing():
        return None

    def z_joined(r, dx, dy):
        mid = recv_xy[r, code((dx, dy, 0))]
        low = turn(recv_xy[r, code((dx, dy, -1))], -7, 1)
        high = turn(recv_xy[r, code((dx, dy, 1))], 7, 1)
        return mid + jnp.where(c8 == 0, low, jnp.where(c8 == 7, high, 0.0))

    def assemble(v, r, between=nothing):
        v = list(v)
        c = v[0].shape[0]
        lower, upper = turn(v[0], 64, 2), turn(v[3], 64, 2)
        v[0] = v[0] + jnp.where((lane < 64) & (row >= 4), turn(upper, 4, 1), 0.0)
        v[3] = v[3] + jnp.where((lane >= 64) & (row < 12), turn(lower, -4, 1), 0.0)
        lower = v[0]
        upper = turn(v[0], 72, 2)
        for t in range(1, 4):
            lower = jnp.where(node_b == t, turn(v[t], 8 * t, 2), lower)
            upper = jnp.where(node_b == t, turn(v[t], 72 + 8 * t, 2), upper)
        d_low = jnp.where(ey > 0, turn(upper, 1, 1), 0.0)
        d_high = jnp.where(ey < 3, turn(lower, -1, 1), 0.0)

        def add_y(d_low, d_high):
            for t in range(4):
                low, high = turn(d_low, -8 * t, 2), turn(d_high, 56 - 8 * t, 2)
                v[t] = v[t] + jnp.where(node_b == 0, low, jnp.where(node_b == 7, high, 0.0))

        add_y(d_low, d_high)
        lower, upper = lower + d_low, upper + d_high
        for side in range(2):
            base = 3 * side
            acc = None
            for k in range(c):
                part = requarter(v[3 * side][k, 8 * side : 8 * side + 8], k, base)
                acc = part if acc is None else jnp.where(quarter == k, part, acc)
            send_x[r, side] = acc
        start(r, c, [d for d in directions if d[0]])
        for side, face in ((0, lower), (1, upper)):
            acc = None
            for k in range(c):
                part = jnp.where(b8 < 4, face[k, 0:8], turn(face[k, 8:16], 32, 1))
                part = turn(part, k + 5 * side, 0)
                acc = part if acc is None else jnp.where(y8 == k, part, acc)
            send_y[r, side] = acc
        start(r, c, [d for d in directions if not d[0] and d[1]])
        lower = v[0]
        upper = turn(v[0], -7, 2)
        for t in range(1, 4):
            lower = jnp.where(node_c == t, turn(v[t], t, 2), lower)
            upper = jnp.where(node_c == t, turn(v[t], t - 7, 2), upper)
        for side, face in ((0, lower), (1, upper)):
            for k in range(c):
                send_z[r, side, k] = jnp.where(c8 < 4, face[k, 0:8], turn(face[k, 8:16], 4, 1))
        start(r, c, [d for d in directions if not d[0] and not d[1]])
        between()
        finish(r, c)
        for side in range(2):
            dx = 2 * side - 1
            low = turn(turn(z_joined(r, dx, -1), -56, 1), -3, 0)
            high = turn(turn(z_joined(r, dx, 1), 56, 1), 3, 0)
            face = z_joined(r, dx, 0) + jnp.where(
                (y8 == 0) & (b8 == 0), low, jnp.where((y8 == 3) & (b8 == 7), high, 0.0)
            )
            base = 3 * side
            parts = [
                jnp.where(quarter == base, requarter(face, k, base), 0.0) for k in range(c)
            ]
            part = jnp.stack(parts)
            zero = jnp.zeros_like(part)
            pair = [part, zero] if side == 0 else [zero, part]
            v[3 * side] = v[3 * side] + jnp.concatenate(pair, axis=1)
        got = []
        for side in range(2):
            face = z_joined(r, 0, 2 * side - 1)
            parts = []
            for k in range(c):
                part = jnp.where(y8 == 3 * side, turn(face, 3 * side - k, 0), 0.0)
                parts.append(jnp.concatenate([part, turn(part, -32, 1)], axis=0))
            got.append(jnp.stack(parts))
        add_y(got[0], got[1])
        got = []
        for side in range(2):
            face = recv_z[r, side, :c]
            got.append(jnp.concatenate([face, turn(face, -4, 2)], axis=1))
        for t in range(4):
            low, high = turn(got[0], -t, 2), turn(got[1], 7 - t, 2)
            v[t] = v[t] + jnp.where(node_c == 0, low, jnp.where(node_c == 7, high, 0.0))
        return v

    def advect(v):
        dx = along_x(0, v)
        dyz = along_lanes(v, fwd_ref)
        return [
            velocity[t][0:1] * dx[t]
            + velocity[t][1:2] * dyz[t][:, :, :128]
            + velocity[t][2:3] * dyz[t][:, :, 128:]
            for t in range(4)
        ]

    first = advect(velocity)
    square_x = along_x(64, mobile)
    square_yz = along_lanes(mobile, sqr_ref)
    diag = [mass_shift * quad[t] + square_x[t] + square_yz[t] for t in range(4)]
    pl.semaphore_wait(barrier, greeted)
    joint = assemble([jnp.concatenate([first[t], diag[t]], axis=0) for t in range(4)], 0)
    inverse_jacobi = [1.0 / joint[t][3:4] for t in range(4)]
    k1 = [joint[t][0:3] * share[t] for t in range(4)]
    total_rate = k1
    v = [velocity[t] - (0.5 * time_step) * k1[t] for t in range(4)]
    for r, step, weight in ((1, 0.5, 2.0), (2, 1.0, 2.0), (3, 0.0, 1.0)):
        g = assemble(advect(v), r)
        g = [g[t] * share[t] for t in range(4)]
        total_rate = [total_rate[t] + weight * g[t] for t in range(4)]
        if step:
            v = [velocity[t] - (step * time_step) * g[t] for t in range(4)]
    advected = [velocity[t] - (time_step / 6.0) * total_rate[t] for t in range(4)]

    dx = along_x(0, [advected[t][0:1] for t in range(4)])
    dyz = along_lanes([advected[t][1:3] for t in range(4)], fwd_ref)
    div = [dx[t] + dyz[t][0:1, :, :128] + dyz[t][1:2, :, 128:] for t in range(4)]
    total_div = assemble(div, 4)
    r0 = [total_div[t] * (quad[t] * (-1.0 / time_step)) for t in range(4)]

    def local(v):
        dx = along_x(0, v)
        dyz = along_lanes(v, fwd_ref)
        gx = [mobile[t] * dx[t] for t in range(4)]
        gyz = [
            jnp.concatenate(
                [mobile[t] * dyz[t][:, :, :128], mobile[t] * dyz[t][:, :, 128:]], axis=2
            )
            for t in range(4)
        ]
        bx = along_x(32, gx)
        byz = along_lanes(gyz, bwd_ref)
        return [(mass_shift * quad[t]) * v[t] + bx[t] + byz[t] for t in range(4)]

    def dot_row(a, b, scale=None):
        acc = None
        for t in range(4):
            term = a[t] * b[t]
            if scale is not None:
                term = term * scale[t]
            acc = term if acc is None else acc + term
        return jnp.sum(acc[0], axis=0, keepdims=True)

    z0 = [r0[t] * inverse_jacobi[t] for t in range(4)]
    lz = local(z0)
    rho_row = dot_row(r0, z0, share)
    gamma_row = dot_row(z0, lz)
    s = assemble(lz, 5)
    w = [s[t] * inverse_jacobi[t] for t in range(4)]
    lw = local(w)
    delta_row = dot_row(s, w, share)
    eps_row = dot_row(w, lw)
    sums[0] = jnp.concatenate(
        [rho_row, gamma_row, delta_row, eps_row, jnp.zeros((4, 128), f32)], axis=0
    )
    sum_bufs = (sums_x, sums_y, sums_z)

    def sum_copy(axis, k):
        return pltpu.make_async_remote_copy(
            src_ref=sums.at[axis],
            dst_ref=sum_bufs[axis].at[k - 1],
            send_sem=sum_send[axis].at[k - 1],
            recv_sem=sum_recv[axis].at[k - 1],
            device_id=at(axis, lax.rem(me[axis] + k, counts[axis])),
            device_id_type=MESH,
        )

    def sum_start(axis):
        for k in range(1, counts[axis]):
            sum_copy(axis, k).start()

    def sum_finish(axis):
        joined = sums[axis]
        for k in range(1, counts[axis]):
            sum_copy(axis, k).wait_recv()
            joined = joined + sum_bufs[axis][k - 1]
        sums[axis + 1] = joined

    def reduce_sums():
        for axis in range(3):
            sum_start(axis)
            sum_finish(axis)

    t_vec = assemble(lw, 6, reduce_sums)
    four = jnp.sum(sums[3], axis=1, keepdims=True)
    rho, gamma, delta, eps = (four[i : i + 1].reshape(1, 1, 1) for i in range(4))
    alpha0 = rho / gamma
    rho1 = rho - 2.0 * alpha0 * gamma + alpha0 * alpha0 * delta
    beta = rho1 / rho
    cross = gamma - alpha0 * delta
    curve = gamma - 2.0 * alpha0 * delta + alpha0 * alpha0 * eps
    curve = curve + 2.0 * beta * cross + beta * beta * gamma
    alpha1 = rho1 / curve
    along = alpha0 + alpha1 * (1.0 + beta)
    side_step = alpha0 * alpha1

    def put(field):
        return order(to_slot, field)

    for i in range(3):
        adv_ref[i] = put(jnp.concatenate([advected[t][i] for t in range(4)], axis=1))
    pre_ref[...] = put(
        jnp.concatenate([(along * z0[t] - side_step * w[t])[0] for t in range(4)], axis=1)
    )
    res_ref[...] = put(
        jnp.concatenate(
            [(r0[t] - along * s[t] + side_step * t_vec[t])[0] for t in range(4)], axis=1
        )
    )
    for r in range(ROUNDS):
        c = 4 if r == 0 else 3 if r < 4 else 1
        for d in directions:

            @pl.when(exists(d))
            def _():
                copy(r, d, c, False).wait_send()

    for axis in range(3):
        for k in range(1, counts[axis]):
            sum_copy(axis, k).wait_send()


def per_device(counts, velocity, inv_density, element_place):
    f32 = jnp.float32
    rows, forward, backward, square = constants()
    elements = element_place.shape[0]
    points = inv_density.shape[0]
    vmem = pl.BlockSpec(memory_space=pltpu.VMEM)
    faces = pltpu.VMEM((ROUNDS, 2, 8, 128), f32)
    faces_z = pltpu.VMEM((ROUNDS, 2, 4, 8, 128), f32)
    dma = pltpu.SemaphoreType.DMA
    peers = [n - 1 for n in counts]
    advected, pressure, residual = pl.pallas_call(
        functools.partial(kernel, counts),
        out_shape=(
            jax.ShapeDtypeStruct((3, elements, points), f32),
            jax.ShapeDtypeStruct((elements, points), f32),
            jax.ShapeDtypeStruct((elements, points), f32),
        ),
        in_specs=[vmem, vmem, pl.BlockSpec(memory_space=pltpu.SMEM), vmem, vmem, vmem, vmem],
        out_specs=(vmem, vmem, vmem),
        scratch_shapes=[
            faces,
            faces,
            faces_z,
            pltpu.VMEM((ROUNDS, 27, 8, 128), f32),
            faces_z,
            pltpu.VMEM((4, 8, 128), f32),
            pltpu.VMEM((peers[0], 8, 128), f32),
            pltpu.VMEM((peers[1], 8, 128), f32),
            pltpu.VMEM((peers[2], 8, 128), f32),
            dma((ROUNDS, 27)),
            dma((ROUNDS, 27)),
            [dma((n,)) for n in peers],
            [dma((n,)) for n in peers],
        ],
        compiler_params=pltpu.CompilerParams(collective_id=0, has_side_effects=True),
    )(
        velocity.transpose(0, 2, 1),
        inv_density.T,
        element_place,
        jnp.asarray(rows),
        jnp.asarray(forward),
        jnp.asarray(backward),
        jnp.asarray(square),
    )
    return advected.transpose(0, 2, 1), pressure.T, residual.T


def solution(mesh):
    counts = tuple(mesh.shape[name] for name in AXES)
    placed = (P(None, None, AXES), P(None, AXES), P(AXES))
    return jax.shard_map(
        functools.partial(per_device, counts),
        mesh=mesh,
        in_specs=placed,
        out_specs=(P(None, None, AXES), P(None, AXES), P(None, AXES)),
        check_vma=False,
    )
```

```python
import functools

import jax
import jax.numpy as jnp
import numpy as np
from jax import lax
from jax.experimental import pallas as pl
from jax.experimental.pallas import tpu as pltpu
from jax.sharding import PartitionSpec as P

BX = 4
BY = 4
BZ = 1
MESH = pl.DeviceIdType.MESH
AXES = ("gx", "gy", "gz")
ROUNDS = 7

time_step = 0.03
mass_shift = 4.0
inner_nodes = (
    -0.8717401485096066,
    -0.5917001814331423,
    -0.2092992179024789,
    0.2092992179024789,
    0.5917001814331423,
    0.8717401485096066,
)


def legendre_seven(position):
    previous = 1.0
    current_value = position
    for degree_index in range(1, 7):
        following = (
            (2 * degree_index + 1) * position * current_value - degree_index * previous
        ) / (degree_index + 1)
        previous = current_value
        current_value = following
    return current_value


def tables():
    nodes = [-1.0] + list(inner_nodes) + [1.0]
    poly = [legendre_seven(node) for node in nodes]
    weights = np.array([2.0 / (56.0 * value * value) for value in poly])
    derivative = np.zeros((8, 8))
    for i in range(8):
        for j in range(8):
            if i != j:
                derivative[i, j] = poly[i] / (poly[j] * (nodes[i] - nodes[j]))
    derivative[0, 0] = -14.0
    derivative[7, 7] = 14.0
    return weights, derivative.astype(np.float32).astype(np.float64)


def lane_rows(matrix):
    rows = np.zeros((32, 128))
    for t in range(4):
        for u in range(4):
            for h in range(2):
                rows[8 * t + 2 * u, 64 * h : 64 * h + 64] = matrix[2 * t + h, 2 * u + h]
                rows[8 * t + 2 * u + 1, 64 * h : 64 * h + 64] = matrix[2 * t + h, 2 * u + 1 - h]
    return rows


def split_stack(matrix):
    high = np.asarray(matrix, np.float32).astype(jnp.bfloat16)
    low = (np.asarray(matrix, np.float32) - high.astype(np.float32)).astype(jnp.bfloat16)
    return np.concatenate([high, high, low], axis=0)


@functools.cache
def constants():
    weights, d = tables()
    eye2, eye8, eye16 = np.eye(2), np.eye(8), np.eye(16)
    forward = np.concatenate(
        [np.kron(np.kron(eye2, d.T), eye8), np.kron(eye16, d.T)], axis=1
    )
    backward = np.concatenate([np.kron(np.kron(eye2, d), eye8), np.kron(eye16, d)], axis=0)
    square = np.kron(np.kron(eye2, d**2), eye8) + np.kron(eye16, d**2)
    quad = np.einsum("a,b,c->abc", weights, weights, weights).reshape(4, 128)
    rows = np.concatenate(
        [lane_rows(d), lane_rows(d.T), lane_rows(d.T**2), quad, np.zeros((4, 128))], axis=0
    )
    return (
        rows.astype(np.float32),
        split_stack(forward),
        split_stack(backward),
        split_stack(square),
    )


def kernel(
    counts,
    vel_ref,
    den_ref,
    place_ref,
    rows_ref,
    fwd_ref,
    bwd_ref,
    sqr_ref,
    adv_ref,
    pre_ref,
    res_ref,
    send_x,
    send_y,
    send_z,
    recv_xy,
    recv_z,
    sums,
    sums_in,
    send_sem,
    recv_sem,
    sum_send,
    sum_recv,
):
    f32 = jnp.float32
    me = [lax.axis_index(name) for name in AXES]
    has = [(me[i] > 0, me[i] < counts[i] - 1) for i in range(3)]

    lane = lax.broadcasted_iota(jnp.int32, (1, 16, 128), 2)
    row = lax.broadcasted_iota(jnp.int32, (1, 16, 128), 1)
    ex, ey = row // BY, row % BY
    node_b, node_c = (lane // 8) % 8, lane % 8

    r16 = lax.broadcasted_iota(jnp.int32, (16, 16), 0)
    l16 = lax.broadcasted_iota(jnp.int32, (16, 16), 1)
    by_lane = jnp.zeros((16, 16), jnp.int32)
    by_row = jnp.zeros((16, 16), jnp.int32)
    for e in range(16):
        by_lane = jnp.where(l16 == e, place_ref[e], by_lane)
        by_row = jnp.where(r16 == e, place_ref[e], by_row)
    to_place = (by_lane == r16).astype(f32)
    to_slot = (by_row == l16).astype(f32)

    def order(matrix, block):
        return jnp.dot(
            matrix, block, precision=lax.Precision.HIGHEST, preferred_element_type=f32
        )

    placed = [order(to_place, vel_ref[i]) for i in range(3)]
    velocity = [
        jnp.stack([placed[i][:, 128 * t : 128 * t + 128] for i in range(3)]) for t in range(4)
    ]
    dens = order(to_place, den_ref[...])
    quad = [rows_ref[96 + t : 97 + t, :].reshape(1, 1, 128) for t in range(4)]
    mobile = [quad[t] * dens[:, 128 * t : 128 * t + 128].reshape(1, 16, 128) for t in range(4)]

    def half(flag):
        return jnp.where(flag, 0.5, 1.0).astype(f32)

    total = [BX * counts[0], BY * counts[1], BZ * counts[2]]
    pos_x, pos_y = ex + me[0] * BX, ey + me[1] * BY
    share_y = half(
        ((node_b == 0) & (pos_y > 0)) | ((node_b == 7) & (pos_y < total[1] - 1))
    )
    pos_z = row * 0 + me[2]
    share_z = half(((node_c == 0) & (pos_z > 0)) | ((node_c == 7) & (pos_z < total[2] - 1)))
    share_yz = share_y * share_z
    share = [share_yz] * 4
    share[0] = share_yz * half((lane < 64) & (pos_x > 0))
    share[3] = share_yz * half((lane >= 64) & (pos_x < total[0] - 1))

    def along_x(base, v):
        swapped = [pltpu.roll(v[t], 64, 2) for t in range(4)]
        out = []
        for t in range(4):
            acc = None
            for u in range(4):
                k = base + 8 * t + 2 * u
                term = (
                    rows_ref[k : k + 1, :].reshape(1, 1, 128) * v[u]
                    + rows_ref[k + 1 : k + 2, :].reshape(1, 1, 128) * swapped[u]
                )
                acc = term if acc is None else acc + term
            out.append(acc)
        return out

    def split(x):
        high = x.astype(jnp.bfloat16)
        low = (x - high.astype(f32)).astype(jnp.bfloat16)
        return jnp.concatenate([high, low, high], axis=1)

    def along_lanes(v, w_ref):
        c = v[0].shape[0]
        x = jnp.concatenate([v[t].reshape(c * 16, -1) for t in range(4)], axis=0)
        y = jnp.dot(split(x), w_ref[...], preferred_element_type=f32)
        return [y[t * c * 16 : (t + 1) * c * 16].reshape(c, 16, -1) for t in range(4)]

    directions = [
        (dx, dy, dz)
        for dx in (-1, 0, 1)
        for dy in (-1, 0, 1)
        for dz in (-1, 0, 1)
        if (dx, dy, dz) != (0, 0, 0)
    ]
    columns = [(dx, dy) for dx in (-1, 1, 0) for dy in (0, -1, 1)]
    cases = []
    if counts[2] > 2:
        cases.append(((-1, 0, 1), jnp.logical_and(has[2][0], has[2][1])))
    if counts[2] > 1:
        cases.append(((-1, 0), jnp.logical_not(has[2][1])))
        cases.append(((0, 1), jnp.logical_not(has[2][0])))
    else:
        cases.append(((0,), me[2] == 0))

    def code(d):
        return (d[0] + 1) * 9 + (d[1] + 1) * 3 + d[2] + 1

    def group(d):
        return (d[0] + 1) * 3 + d[1] + 1 if d[0] or d[1] else 9 + side_of(d[2])

    def exists(d):
        flag = None
        for i in range(3):
            if d[i]:
                here = has[i][1 if d[i] > 0 else 0]
                flag = here if flag is None else jnp.logical_and(flag, here)
        return flag

    def side_of(step):
        return 1 if step > 0 else 0

    def source(r, d, c):
        if d[0]:
            return send_x.at[r, side_of(d[0])]
        if d[1]:
            return send_y.at[r, side_of(d[1])]
        return send_z.at[r, side_of(d[2]), pl.ds(0, c)]

    def target(r, d, c):
        if d[0] or d[1]:
            return recv_xy.at[r, code(d)]
        return recv_z.at[r, side_of(d[2]), pl.ds(0, c)]

    def copy(r, d, c, incoming):
        back = d if incoming else tuple(-i for i in d)
        return pltpu.make_async_remote_copy(
            src_ref=source(r, d, c),
            dst_ref=target(r, back, c),
            send_sem=send_sem.at[group(d)],
            recv_sem=recv_sem.at[r, group(back)],
            device_id=tuple(me[i] + d[i] for i in range(3)),
            device_id_type=MESH,
        )

    def each_column(act):
        for steps, flag in cases:

            @pl.when(flag)
            def _():
                for dx, dy in columns:
                    if dx or dy:

                        @pl.when(exists((dx, dy, 0)))
                        def _():
                            act(dx, dy, steps)

                    else:
                        act(dx, dy, [dz for dz in steps if dz])

    def start(r, c):
        def act(dx, dy, steps):
            for dz in steps:
                copy(r, (dx, dy, dz), c, False).start()

        each_column(act)

    def whole(ref, d, rounds_sem):
        return pltpu.make_async_remote_copy(
            src_ref=ref,
            dst_ref=ref,
            send_sem=send_sem.at[group(d)],
            recv_sem=rounds_sem.at[group(d)],
            device_id=tuple(me[i] + d[i] for i in range(3)),
            device_id_type=MESH,
        )

    def finish(r, c):
        def act(dx, dy, steps):
            if dx or dy:
                d = (dx, dy, 0)
                ref = recv_xy.at[r, pl.ds(code((dx, dy, steps[0])), len(steps))]
                whole(ref, d, recv_sem.at[r]).wait_recv()
            else:
                for dz in steps:
                    copy(r, (0, 0, dz), c, True).wait_recv()

        each_column(act)

    def sent():
        def act(dx, dy, steps):
            if dx or dy:
                d = (dx, dy, 0)
                ref = recv_xy.at[:, pl.ds(code((dx, dy, steps[0])), len(steps))]
                whole(ref, d, recv_sem.at[0]).wait_send()
            else:
                for dz in steps:
                    whole(recv_z.at[pl.ds(0, 2)], (0, 0, dz), recv_sem.at[0]).wait_send()

        each_column(act)

    def each_other(act):
        for kx in range(counts[0]):
            for ky in range(counts[1]):
                base = (kx * counts[1] + ky) * counts[2]
                first = 0 if base else 1

                def one(kz, _):
                    steps = (kx, ky, kz)
                    device = tuple(lax.rem(me[i] + steps[i], counts[i]) for i in range(3))
                    act(device, base + kz - 1)
                    return 0

                if counts[2] <= 8:
                    for kz in range(first, counts[2]):
                        one(kz, 0)
                else:
                    lax.fori_loop(first, counts[2], one, 0)

    barrier = pltpu.get_barrier_semaphore()

    def greet(device, index):
        pl.semaphore_signal(barrier, inc=1, device_id=device, device_id_type=MESH)

    each_other(greet)
    others = counts[0] * counts[1] * counts[2] - 1
    for d in directions:

        @pl.when(jnp.logical_not(exists(d)))
        def _():
            for r in range(ROUNDS):
                if d[0] or d[1]:
                    recv_xy[r, code(d)] = jnp.zeros((8, 128), f32)
                else:
                    recv_z[r, side_of(d[2])] = jnp.zeros((4, 8, 128), f32)

    sub8 = lax.broadcasted_iota(jnp.int32, (8, 128), 0)
    lane8 = lax.broadcasted_iota(jnp.int32, (8, 128), 1)
    quarter = sub8 // 4 + 2 * (lane8 // 64)
    b8, c8, y8 = (lane8 // 8) % 8, lane8 % 8, sub8 % 4

    def turn(x, shift, axis):
        size = x.shape[axis]
        shift = shift % size
        return pltpu.roll(x, shift, axis) if shift else x

    def requarter(x, k, base):
        if (k ^ base) & 1:
            x = turn(x, 4, 0)
        if (k ^ base) & 2:
            x = turn(x, 64, 1)
        return x

    def z_joined(r, dx, dy):
        mid = recv_xy[r, code((dx, dy, 0))]
        low = turn(recv_xy[r, code((dx, dy, -1))], -7, 1)
        high = turn(recv_xy[r, code((dx, dy, 1))], 7, 1)
        return mid + jnp.where(c8 == 0, low, jnp.where(c8 == 7, high, 0.0))

    def assemble(v, r):
        v = list(v)
        c = v[0].shape[0]
        lower, upper = turn(v[0], 64, 2), turn(v[3], 64, 2)
        v[0] = v[0] + jnp.where((lane < 64) & (row >= 4), turn(upper, 4, 1), 0.0)
        v[3] = v[3] + jnp.where((lane >= 64) & (row < 12), turn(lower, -4, 1), 0.0)
        lower = v[0]
        upper = turn(v[0], 72, 2)
        for t in range(1, 4):
            lower = jnp.where(node_b == t, turn(v[t], 8 * t, 2), lower)
            upper = jnp.where(node_b == t, turn(v[t], 72 + 8 * t, 2), upper)
        d_low = jnp.where(ey > 0, turn(upper, 1, 1), 0.0)
        d_high = jnp.where(ey < 3, turn(lower, -1, 1), 0.0)

        def add_y(d_low, d_high):
            for t in range(4):
                low, high = turn(d_low, -8 * t, 2), turn(d_high, 56 - 8 * t, 2)
                v[t] = v[t] + jnp.where(node_b == 0, low, jnp.where(node_b == 7, high, 0.0))

        add_y(d_low, d_high)
        lower, upper = lower + d_low, upper + d_high
        for side in range(2):
            base = 3 * side
            acc = None
            for k in range(c):
                part = requarter(v[3 * side][k, 8 * side : 8 * side + 8], k, base)
                acc = part if acc is None else jnp.where(quarter == k, part, acc)
            send_x[r, side] = acc
        for side, face in ((0, lower), (1, upper)):
            acc = None
            for k in range(c):
                part = jnp.where(b8 < 4, face[k, 0:8], turn(face[k, 8:16], 32, 1))
                part = turn(part, k + 5 * side, 0)
                acc = part if acc is None else jnp.where(y8 == k, part, acc)
            send_y[r, side] = acc
        lower = v[0]
        upper = turn(v[0], -7, 2)
        for t in range(1, 4):
            lower = jnp.where(node_c == t, turn(v[t], t, 2), lower)
            upper = jnp.where(node_c == t, turn(v[t], t - 7, 2), upper)
        for side, face in ((0, lower), (1, upper)):
            for k in range(c):
                send_z[r, side, k] = jnp.where(c8 < 4, face[k, 0:8], turn(face[k, 8:16], 4, 1))
        start(r, c)
        finish(r, c)
        for side in range(2):
            dx = 2 * side - 1
            low = turn(turn(z_joined(r, dx, -1), -56, 1), -3, 0)
            high = turn(turn(z_joined(r, dx, 1), 56, 1), 3, 0)
            face = z_joined(r, dx, 0) + jnp.where(
                (y8 == 0) & (b8 == 0), low, jnp.where((y8 == 3) & (b8 == 7), high, 0.0)
            )
            base = 3 * side
            parts = [
                jnp.where(quarter == base, requarter(face, k, base), 0.0) for k in range(c)
            ]
            part = jnp.stack(parts)
            zero = jnp.zeros_like(part)
            pair = [part, zero] if side == 0 else [zero, part]
            v[3 * side] = v[3 * side] + jnp.concatenate(pair, axis=1)
        got = []
        for side in range(2):
            face = z_joined(r, 0, 2 * side - 1)
            parts = []
            for k in range(c):
                part = jnp.where(y8 == 3 * side, turn(face, 3 * side - k, 0), 0.0)
                parts.append(jnp.concatenate([part, turn(part, -32, 1)], axis=0))
            got.append(jnp.stack(parts))
        add_y(got[0], got[1])
        got = []
        for side in range(2):
            face = recv_z[r, side, :c]
            got.append(jnp.concatenate([face, turn(face, -4, 2)], axis=1))
        for t in range(4):
            low, high = turn(got[0], -t, 2), turn(got[1], 7 - t, 2)
            v[t] = v[t] + jnp.where(node_c == 0, low, jnp.where(node_c == 7, high, 0.0))
        return v

    def advect(v):
        dx = along_x(0, v)
        dyz = along_lanes(v, fwd_ref)
        return [
            velocity[t][0:1] * dx[t]
            + velocity[t][1:2] * dyz[t][:, :, :128]
            + velocity[t][2:3] * dyz[t][:, :, 128:]
            for t in range(4)
        ]

    first = advect(velocity)
    square_x = along_x(64, mobile)
    square_yz = along_lanes(mobile, sqr_ref)
    diag = [mass_shift * quad[t] + square_x[t] + square_yz[t] for t in range(4)]
    pl.semaphore_wait(barrier, others)
    joint = assemble([jnp.concatenate([first[t], diag[t]], axis=0) for t in range(4)], 0)
    inverse_jacobi = [1.0 / joint[t][3:4] for t in range(4)]
    k1 = [joint[t][0:3] * share[t] for t in range(4)]
    total_rate = k1
    v = [velocity[t] - (0.5 * time_step) * k1[t] for t in range(4)]
    for r, step, weight in ((1, 0.5, 2.0), (2, 1.0, 2.0), (3, 0.0, 1.0)):
        g = assemble(advect(v), r)
        g = [g[t] * share[t] for t in range(4)]
        total_rate = [total_rate[t] + weight * g[t] for t in range(4)]
        if step:
            v = [velocity[t] - (step * time_step) * g[t] for t in range(4)]
    advected = [velocity[t] - (time_step / 6.0) * total_rate[t] for t in range(4)]

    dx = along_x(0, [advected[t][0:1] for t in range(4)])
    dyz = along_lanes([advected[t][1:3] for t in range(4)], fwd_ref)
    div = [dx[t] + dyz[t][0:1, :, :128] + dyz[t][1:2, :, 128:] for t in range(4)]
    total_div = assemble(div, 4)
    r0 = [total_div[t] * (quad[t] * (-1.0 / time_step)) for t in range(4)]

    def local(v):
        dx = along_x(0, v)
        dyz = along_lanes(v, fwd_ref)
        gx = [mobile[t] * dx[t] for t in range(4)]
        gyz = [
            jnp.concatenate(
                [mobile[t] * dyz[t][:, :, :128], mobile[t] * dyz[t][:, :, 128:]], axis=2
            )
            for t in range(4)
        ]
        bx = along_x(32, gx)
        byz = along_lanes(gyz, bwd_ref)
        return [(mass_shift * quad[t]) * v[t] + bx[t] + byz[t] for t in range(4)]

    def dot_row(a, b, scale=None):
        acc = None
        for t in range(4):
            term = a[t] * b[t]
            if scale is not None:
                term = term * scale[t]
            acc = term if acc is None else acc + term
        return jnp.sum(acc[0], axis=0, keepdims=True)

    z0 = [r0[t] * inverse_jacobi[t] for t in range(4)]
    lz = local(z0)
    rho_row = dot_row(r0, z0, share)
    gamma_row = dot_row(z0, lz)
    s = assemble(lz, 5)
    w = [s[t] * inverse_jacobi[t] for t in range(4)]
    lw = local(w)
    delta_row = dot_row(s, w, share)
    eps_row = dot_row(w, lw)
    partial = jnp.concatenate(
        [rho_row, gamma_row, delta_row, eps_row, jnp.zeros((4, 128), f32)], axis=0
    )
    partial = jnp.sum(partial, axis=1, keepdims=True)
    own = jnp.sum(jnp.where(sub8 == lane8, partial, 0.0), axis=0, keepdims=True)
    sums[...] = own

    def share_sums(device, index):
        pltpu.make_async_remote_copy(
            src_ref=sums,
            dst_ref=sums_in.at[index],
            send_sem=sum_send,
            recv_sem=sum_recv,
            device_id=device,
            device_id_type=MESH,
        ).start()

    each_other(share_sums)
    t_vec = assemble(lw, 6)
    arrived = pltpu.make_async_remote_copy(
        src_ref=sums_in,
        dst_ref=sums_in,
        send_sem=sum_send,
        recv_sem=sum_recv,
        device_id=tuple(lax.rem(me[i] + 1, counts[i]) for i in range(3)),
        device_id_type=MESH,
    )
    arrived.wait_recv()
    joined = own + jnp.sum(sums_in[...], axis=0)
    four = jnp.sum(jnp.where(sub8 == lane8, joined, 0.0), axis=1, keepdims=True)
    rho, gamma, delta, eps = (four[i : i + 1].reshape(1, 1, 1) for i in range(4))
    alpha0 = rho / gamma
    rho1 = rho - 2.0 * alpha0 * gamma + alpha0 * alpha0 * delta
    beta = rho1 / rho
    cross = gamma - alpha0 * delta
    curve = gamma - 2.0 * alpha0 * delta + alpha0 * alpha0 * eps
    curve = curve + 2.0 * beta * cross + beta * beta * gamma
    alpha1 = rho1 / curve
    along = alpha0 + alpha1 * (1.0 + beta)
    side_step = alpha0 * alpha1

    def put(field):
        return order(to_slot, field)

    for i in range(3):
        adv_ref[i] = put(jnp.concatenate([advected[t][i] for t in range(4)], axis=1))
    pre_ref[...] = put(
        jnp.concatenate([(along * z0[t] - side_step * w[t])[0] for t in range(4)], axis=1)
    )
    res_ref[...] = put(
        jnp.concatenate(
            [(r0[t] - along * s[t] + side_step * t_vec[t])[0] for t in range(4)], axis=1
        )
    )
    sent()
    arrived.wait_send()


def per_device(counts, velocity, inv_density, element_place):
    f32 = jnp.float32
    rows, forward, backward, square = constants()
    elements = element_place.shape[0]
    points = inv_density.shape[0]
    vmem = pl.BlockSpec(memory_space=pltpu.VMEM)
    faces = pltpu.VMEM((ROUNDS, 2, 8, 128), f32)
    faces_z = pltpu.VMEM((ROUNDS, 2, 4, 8, 128), f32)
    dma = pltpu.SemaphoreType.DMA
    others = counts[0] * counts[1] * counts[2] - 1
    advected, pressure, residual = pl.pallas_call(
        functools.partial(kernel, counts),
        out_shape=(
            jax.ShapeDtypeStruct((3, elements, points), f32),
            jax.ShapeDtypeStruct((elements, points), f32),
            jax.ShapeDtypeStruct((elements, points), f32),
        ),
        in_specs=[vmem, vmem, pl.BlockSpec(memory_space=pltpu.SMEM), vmem, vmem, vmem, vmem],
        out_specs=(vmem, vmem, vmem),
        scratch_shapes=[
            faces,
            faces,
            faces_z,
            pltpu.VMEM((ROUNDS, 27, 8, 128), f32),
            faces_z,
            pltpu.VMEM((1, 128), f32),
            pltpu.VMEM((others, 1, 128), f32),
            dma((11,)),
            dma((ROUNDS, 11)),
            dma,
            dma,
        ],
        compiler_params=pltpu.CompilerParams(collective_id=0, has_side_effects=True),
    )(
        velocity.transpose(0, 2, 1),
        inv_density.T,
        element_place,
        jnp.asarray(rows),
        jnp.asarray(forward),
        jnp.asarray(backward),
        jnp.asarray(square),
    )
    return advected.transpose(0, 2, 1), pressure.T, residual.T


def solution(mesh):
    counts = tuple(mesh.shape[name] for name in AXES)
    placed = (P(None, None, AXES), P(None, AXES), P(AXES))
    return jax.shard_map(
        functools.partial(per_device, counts),
        mesh=mesh,
        in_specs=placed,
        out_specs=(P(None, None, AXES), P(None, AXES), P(None, AXES)),
        check_vma=False,
    )
```

```python
import functools

import jax
import jax.numpy as jnp
import numpy as np
from jax import lax
from jax.experimental import pallas as pl
from jax.experimental.pallas import tpu as pltpu
from jax.sharding import PartitionSpec as P

BX = 4
BY = 4
BZ = 1
MESH = pl.DeviceIdType.MESH
AXES = ("gx", "gy", "gz")
ROUNDS = 7

time_step = 0.03
mass_shift = 4.0
inner_nodes = (
    -0.8717401485096066,
    -0.5917001814331423,
    -0.2092992179024789,
    0.2092992179024789,
    0.5917001814331423,
    0.8717401485096066,
)


def legendre_seven(position):
    previous = 1.0
    current_value = position
    for degree_index in range(1, 7):
        following = (
            (2 * degree_index + 1) * position * current_value - degree_index * previous
        ) / (degree_index + 1)
        previous = current_value
        current_value = following
    return current_value


def tables():
    nodes = [-1.0] + list(inner_nodes) + [1.0]
    poly = [legendre_seven(node) for node in nodes]
    weights = np.array([2.0 / (56.0 * value * value) for value in poly])
    derivative = np.zeros((8, 8))
    for i in range(8):
        for j in range(8):
            if i != j:
                derivative[i, j] = poly[i] / (poly[j] * (nodes[i] - nodes[j]))
    derivative[0, 0] = -14.0
    derivative[7, 7] = 14.0
    return weights, derivative.astype(np.float32).astype(np.float64)


def lane_rows(matrix):
    rows = np.zeros((32, 128))
    for t in range(4):
        for u in range(4):
            for h in range(2):
                rows[8 * t + 2 * u, 64 * h : 64 * h + 64] = matrix[2 * t + h, 2 * u + h]
                rows[8 * t + 2 * u + 1, 64 * h : 64 * h + 64] = matrix[2 * t + h, 2 * u + 1 - h]
    return rows


def split_stack(matrix):
    high = np.asarray(matrix, np.float32).astype(jnp.bfloat16)
    low = (np.asarray(matrix, np.float32) - high.astype(np.float32)).astype(jnp.bfloat16)
    return np.concatenate([high, high, low], axis=0)


@functools.cache
def constants():
    weights, d = tables()
    eye2, eye8, eye16 = np.eye(2), np.eye(8), np.eye(16)
    forward = np.concatenate(
        [np.kron(np.kron(eye2, d.T), eye8), np.kron(eye16, d.T)], axis=1
    )
    backward = np.concatenate([np.kron(np.kron(eye2, d), eye8), np.kron(eye16, d)], axis=0)
    square = np.kron(np.kron(eye2, d**2), eye8) + np.kron(eye16, d**2)
    quad = np.einsum("a,b,c->abc", weights, weights, weights).reshape(4, 128)
    rows = np.concatenate(
        [lane_rows(d), lane_rows(d.T), lane_rows(d.T**2), quad, np.zeros((4, 128))], axis=0
    )
    return (
        rows.astype(np.float32),
        split_stack(forward),
        split_stack(backward),
        split_stack(square),
    )


def kernel(
    counts,
    vel_ref,
    den_ref,
    place_ref,
    rows_ref,
    fwd_ref,
    bwd_ref,
    sqr_ref,
    adv_ref,
    pre_ref,
    res_ref,
    send_x,
    send_y,
    send_z,
    recv_xy,
    recv_z,
    sums,
    sums_in,
    send_sem,
    recv_sem,
    sum_send,
    sum_recv,
):
    f32 = jnp.float32
    me = [lax.axis_index(name) for name in AXES]
    has = [(me[i] > 0, me[i] < counts[i] - 1) for i in range(3)]

    def each_other(act):
        for kx in range(counts[0]):
            for ky in range(counts[1]):
                base = (kx * counts[1] + ky) * counts[2]
                first = 0 if base else 1

                def one(kz, _):
                    steps = (kx, ky, kz)
                    device = tuple(lax.rem(me[i] + steps[i], counts[i]) for i in range(3))
                    act(device, base + kz - 1)
                    return 0

                if counts[2] <= 8:
                    for kz in range(first, counts[2]):
                        one(kz, 0)
                else:
                    lax.fori_loop(first, counts[2], one, 0)

    barrier = pltpu.get_barrier_semaphore()

    def greet(device, index):
        pl.semaphore_signal(barrier, inc=1, device_id=device, device_id_type=MESH)

    each_other(greet)
    others = counts[0] * counts[1] * counts[2] - 1

    lane = lax.broadcasted_iota(jnp.int32, (1, 16, 128), 2)
    row = lax.broadcasted_iota(jnp.int32, (1, 16, 128), 1)
    ex, ey = row // BY, row % BY
    node_b, node_c = (lane // 8) % 8, lane % 8

    r16 = lax.broadcasted_iota(jnp.int32, (16, 16), 0)
    l16 = lax.broadcasted_iota(jnp.int32, (16, 16), 1)
    by_lane = jnp.zeros((16, 16), jnp.int32)
    by_row = jnp.zeros((16, 16), jnp.int32)
    for e in range(16):
        by_lane = jnp.where(l16 == e, place_ref[e], by_lane)
        by_row = jnp.where(r16 == e, place_ref[e], by_row)
    to_place = (by_lane == r16).astype(f32)
    to_slot = (by_row == l16).astype(f32)

    def order(matrix, block):
        return jnp.dot(
            matrix, block, precision=lax.Precision.HIGHEST, preferred_element_type=f32
        )

    placed = [order(to_place, vel_ref[i]) for i in range(3)]
    velocity = [
        jnp.stack([placed[i][:, 128 * t : 128 * t + 128] for i in range(3)]) for t in range(4)
    ]
    dens = order(to_place, den_ref[...])
    quad = [rows_ref[96 + t : 97 + t, :].reshape(1, 1, 128) for t in range(4)]
    mobile = [quad[t] * dens[:, 128 * t : 128 * t + 128].reshape(1, 16, 128) for t in range(4)]

    def half(flag):
        return jnp.where(flag, 0.5, 1.0).astype(f32)

    total = [BX * counts[0], BY * counts[1], BZ * counts[2]]
    pos_x, pos_y = ex + me[0] * BX, ey + me[1] * BY
    share_y = half(
        ((node_b == 0) & (pos_y > 0)) | ((node_b == 7) & (pos_y < total[1] - 1))
    )
    pos_z = row * 0 + me[2]
    share_z = half(((node_c == 0) & (pos_z > 0)) | ((node_c == 7) & (pos_z < total[2] - 1)))
    share_yz = share_y * share_z
    share = [share_yz] * 4
    share[0] = share_yz * half((lane < 64) & (pos_x > 0))
    share[3] = share_yz * half((lane >= 64) & (pos_x < total[0] - 1))

    def along_x(base, v):
        swapped = [pltpu.roll(v[t], 64, 2) for t in range(4)]
        out = []
        for t in range(4):
            acc = None
            for u in range(4):
                k = base + 8 * t + 2 * u
                term = (
                    rows_ref[k : k + 1, :].reshape(1, 1, 128) * v[u]
                    + rows_ref[k + 1 : k + 2, :].reshape(1, 1, 128) * swapped[u]
                )
                acc = term if acc is None else acc + term
            out.append(acc)
        return out

    def split(x):
        high = x.astype(jnp.bfloat16)
        low = (x - high.astype(f32)).astype(jnp.bfloat16)
        return jnp.concatenate([high, low, high], axis=1)

    def along_lanes(v, w_ref):
        c = v[0].shape[0]
        x = jnp.concatenate([v[t].reshape(c * 16, -1) for t in range(4)], axis=0)
        y = jnp.dot(split(x), w_ref[...], preferred_element_type=f32)
        return [y[t * c * 16 : (t + 1) * c * 16].reshape(c, 16, -1) for t in range(4)]

    directions = [
        (dx, dy, dz)
        for dx in (-1, 0, 1)
        for dy in (-1, 0, 1)
        for dz in (-1, 0, 1)
        if (dx, dy, dz) != (0, 0, 0)
    ]
    columns = [(dx, dy) for dx in (-1, 1, 0) for dy in (0, -1, 1)]
    cases = []
    if counts[2] > 2:
        cases.append(((-1, 0, 1), jnp.logical_and(has[2][0], has[2][1])))
    if counts[2] > 1:
        cases.append(((-1, 0), jnp.logical_not(has[2][1])))
        cases.append(((0, 1), jnp.logical_not(has[2][0])))
    else:
        cases.append(((0,), me[2] == 0))

    def code(d):
        return (d[0] + 1) * 9 + (d[1] + 1) * 3 + d[2] + 1

    def group(d):
        return (d[0] + 1) * 3 + d[1] + 1 if d[0] or d[1] else 9 + side_of(d[2])

    def exists(d):
        flag = None
        for i in range(3):
            if d[i]:
                here = has[i][1 if d[i] > 0 else 0]
                flag = here if flag is None else jnp.logical_and(flag, here)
        return flag

    def side_of(step):
        return 1 if step > 0 else 0

    def source(r, d, c):
        if d[0]:
            return send_x.at[r, side_of(d[0])]
        if d[1]:
            return send_y.at[r, side_of(d[1])]
        return send_z.at[r, side_of(d[2]), pl.ds(0, c)]

    def target(r, d, c):
        if d[0] or d[1]:
            return recv_xy.at[r, code(d)]
        return recv_z.at[r, side_of(d[2]), pl.ds(0, c)]

    def copy(r, d, c, incoming):
        back = d if incoming else tuple(-i for i in d)
        return pltpu.make_async_remote_copy(
            src_ref=source(r, d, c),
            dst_ref=target(r, back, c),
            send_sem=send_sem.at[group(d)],
            recv_sem=recv_sem.at[r, group(back)],
            device_id=tuple(me[i] + d[i] for i in range(3)),
            device_id_type=MESH,
        )

    def each_column(act):
        for steps, flag in cases:

            @pl.when(flag)
            def _():
                for dx, dy in columns:
                    if dx or dy:

                        @pl.when(exists((dx, dy, 0)))
                        def _():
                            act(dx, dy, steps)

                    else:
                        act(dx, dy, [dz for dz in steps if dz])

    def start(r, c):
        def act(dx, dy, steps):
            for dz in steps:
                copy(r, (dx, dy, dz), c, False).start()

        each_column(act)

    def whole(ref, d, rounds_sem):
        return pltpu.make_async_remote_copy(
            src_ref=ref,
            dst_ref=ref,
            send_sem=send_sem.at[group(d)],
            recv_sem=rounds_sem.at[group(d)],
            device_id=tuple(me[i] + d[i] for i in range(3)),
            device_id_type=MESH,
        )

    def finish(r, c):
        def act(dx, dy, steps):
            if dx or dy:
                d = (dx, dy, 0)
                ref = recv_xy.at[r, pl.ds(code((dx, dy, steps[0])), len(steps))]
                whole(ref, d, recv_sem.at[r]).wait_recv()
            else:
                for dz in steps:
                    copy(r, (0, 0, dz), c, True).wait_recv()

        each_column(act)

    def sent():
        def act(dx, dy, steps):
            if dx or dy:
                d = (dx, dy, 0)
                ref = recv_xy.at[:, pl.ds(code((dx, dy, steps[0])), len(steps))]
                whole(ref, d, recv_sem.at[0]).wait_send()
            else:
                for dz in steps:
                    whole(recv_z.at[pl.ds(0, 2)], (0, 0, dz), recv_sem.at[0]).wait_send()

        each_column(act)

    for d in directions:

        @pl.when(jnp.logical_not(exists(d)))
        def _():
            for r in range(ROUNDS):
                if d[0] or d[1]:
                    recv_xy[r, code(d)] = jnp.zeros((8, 128), f32)
                else:
                    recv_z[r, side_of(d[2])] = jnp.zeros((4, 8, 128), f32)

    sub8 = lax.broadcasted_iota(jnp.int32, (8, 128), 0)
    lane8 = lax.broadcasted_iota(jnp.int32, (8, 128), 1)
    quarter = sub8 // 4 + 2 * (lane8 // 64)
    b8, c8, y8 = (lane8 // 8) % 8, lane8 % 8, sub8 % 4

    def turn(x, shift, axis):
        size = x.shape[axis]
        shift = shift % size
        return pltpu.roll(x, shift, axis) if shift else x

    def requarter(x, k, base):
        if (k ^ base) & 1:
            x = turn(x, 4, 0)
        if (k ^ base) & 2:
            x = turn(x, 64, 1)
        return x

    def z_joined(r, dx, dy):
        mid = recv_xy[r, code((dx, dy, 0))]
        low = turn(recv_xy[r, code((dx, dy, -1))], -7, 1)
        high = turn(recv_xy[r, code((dx, dy, 1))], 7, 1)
        return mid + jnp.where(c8 == 0, low, jnp.where(c8 == 7, high, 0.0))

    def assemble(v, r, hook=None):
        v = list(v)
        c = v[0].shape[0]
        lower, upper = turn(v[0], 64, 2), turn(v[3], 64, 2)
        v[0] = v[0] + jnp.where((lane < 64) & (row >= 4), turn(upper, 4, 1), 0.0)
        v[3] = v[3] + jnp.where((lane >= 64) & (row < 12), turn(lower, -4, 1), 0.0)
        lower = v[0]
        upper = turn(v[0], 72, 2)
        for t in range(1, 4):
            lower = jnp.where(node_b == t, turn(v[t], 8 * t, 2), lower)
            upper = jnp.where(node_b == t, turn(v[t], 72 + 8 * t, 2), upper)
        d_low = jnp.where(ey > 0, turn(upper, 1, 1), 0.0)
        d_high = jnp.where(ey < 3, turn(lower, -1, 1), 0.0)

        def add_y(d_low, d_high):
            for t in range(4):
                low, high = turn(d_low, -8 * t, 2), turn(d_high, 56 - 8 * t, 2)
                v[t] = v[t] + jnp.where(node_b == 0, low, jnp.where(node_b == 7, high, 0.0))

        add_y(d_low, d_high)
        lower, upper = lower + d_low, upper + d_high
        for side in range(2):
            base = 3 * side
            acc = None
            for k in range(c):
                part = requarter(v[3 * side][k, 8 * side : 8 * side + 8], k, base)
                acc = part if acc is None else jnp.where(quarter == k, part, acc)
            send_x[r, side] = acc
        for side, face in ((0, lower), (1, upper)):
            acc = None
            for k in range(c):
                part = jnp.where(b8 < 4, face[k, 0:8], turn(face[k, 8:16], 32, 1))
                part = turn(part, k + 5 * side, 0)
                acc = part if acc is None else jnp.where(y8 == k, part, acc)
            send_y[r, side] = acc
        lower = v[0]
        upper = turn(v[0], -7, 2)
        for t in range(1, 4):
            lower = jnp.where(node_c == t, turn(v[t], t, 2), lower)
            upper = jnp.where(node_c == t, turn(v[t], t - 7, 2), upper)
        for side, face in ((0, lower), (1, upper)):
            for k in range(c):
                send_z[r, side, k] = jnp.where(c8 < 4, face[k, 0:8], turn(face[k, 8:16], 4, 1))
        start(r, c)
        if hook is not None:
            hook()
        finish(r, c)
        for side in range(2):
            dx = 2 * side - 1
            low = turn(turn(z_joined(r, dx, -1), -56, 1), -3, 0)
            high = turn(turn(z_joined(r, dx, 1), 56, 1), 3, 0)
            face = z_joined(r, dx, 0) + jnp.where(
                (y8 == 0) & (b8 == 0), low, jnp.where((y8 == 3) & (b8 == 7), high, 0.0)
            )
            base = 3 * side
            parts = [
                jnp.where(quarter == base, requarter(face, k, base), 0.0) for k in range(c)
            ]
            part = jnp.stack(parts)
            zero = jnp.zeros_like(part)
            pair = [part, zero] if side == 0 else [zero, part]
            v[3 * side] = v[3 * side] + jnp.concatenate(pair, axis=1)
        got = []
        for side in range(2):
            face = z_joined(r, 0, 2 * side - 1)
            parts = []
            for k in range(c):
                part = jnp.where(y8 == 3 * side, turn(face, 3 * side - k, 0), 0.0)
                parts.append(jnp.concatenate([part, turn(part, -32, 1)], axis=0))
            got.append(jnp.stack(parts))
        add_y(got[0], got[1])
        got = []
        for side in range(2):
            face = recv_z[r, side, :c]
            got.append(jnp.concatenate([face, turn(face, -4, 2)], axis=1))
        for t in range(4):
            low, high = turn(got[0], -t, 2), turn(got[1], 7 - t, 2)
            v[t] = v[t] + jnp.where(node_c == 0, low, jnp.where(node_c == 7, high, 0.0))
        return v

    def advect(v):
        dx = along_x(0, v)
        dyz = along_lanes(v, fwd_ref)
        return [
            velocity[t][0:1] * dx[t]
            + velocity[t][1:2] * dyz[t][:, :, :128]
            + velocity[t][2:3] * dyz[t][:, :, 128:]
            for t in range(4)
        ]

    first = advect(velocity)
    diag = []

    def diagonal():
        square_x = along_x(64, mobile)
        square_yz = along_lanes(mobile, sqr_ref)
        diag.extend(mass_shift * quad[t] + square_x[t] + square_yz[t] for t in range(4))

    pl.semaphore_wait(barrier, others)
    first = assemble(first, 0, diagonal)
    k1 = [first[t] * share[t] for t in range(4)]
    total_rate = k1
    v = [velocity[t] - (0.5 * time_step) * k1[t] for t in range(4)]
    for r, step, weight in ((1, 0.5, 2.0), (2, 1.0, 2.0), (3, 0.0, 1.0)):
        g = advect(v)
        if r == 1:
            g = assemble([jnp.concatenate([g[t], diag[t]], axis=0) for t in range(4)], r)
            inverse_jacobi = [1.0 / g[t][3:4] for t in range(4)]
            g = [g[t][0:3] for t in range(4)]
        else:
            g = assemble(g, r)
        g = [g[t] * share[t] for t in range(4)]
        total_rate = [total_rate[t] + weight * g[t] for t in range(4)]
        if step:
            v = [velocity[t] - (step * time_step) * g[t] for t in range(4)]
    advected = [velocity[t] - (time_step / 6.0) * total_rate[t] for t in range(4)]

    dx = along_x(0, [advected[t][0:1] for t in range(4)])
    dyz = along_lanes([advected[t][1:3] for t in range(4)], fwd_ref)
    div = [dx[t] + dyz[t][0:1, :, :128] + dyz[t][1:2, :, 128:] for t in range(4)]
    def put(field):
        return order(to_slot, field)

    def put_advected():
        for i in range(3):
            adv_ref[i] = put(jnp.concatenate([advected[t][i] for t in range(4)], axis=1))

    total_div = assemble(div, 4, put_advected)
    r0 = [total_div[t] * (quad[t] * (-1.0 / time_step)) for t in range(4)]

    def local(v):
        dx = along_x(0, v)
        dyz = along_lanes(v, fwd_ref)
        gx = [mobile[t] * dx[t] for t in range(4)]
        gyz = [
            jnp.concatenate(
                [mobile[t] * dyz[t][:, :, :128], mobile[t] * dyz[t][:, :, 128:]], axis=2
            )
            for t in range(4)
        ]
        bx = along_x(32, gx)
        byz = along_lanes(gyz, bwd_ref)
        return [(mass_shift * quad[t]) * v[t] + bx[t] + byz[t] for t in range(4)]

    def dot_row(a, b, scale=None):
        acc = None
        for t in range(4):
            term = a[t] * b[t]
            if scale is not None:
                term = term * scale[t]
            acc = term if acc is None else acc + term
        return jnp.sum(acc[0], axis=0, keepdims=True)

    z0 = [r0[t] * inverse_jacobi[t] for t in range(4)]
    lz = local(z0)
    rho_row = dot_row(r0, z0, share)
    gamma_row = dot_row(z0, lz)
    s = assemble(lz, 5)
    w = [s[t] * inverse_jacobi[t] for t in range(4)]
    lw = local(w)
    delta_row = dot_row(s, w, share)
    eps_row = dot_row(w, lw)
    partial = jnp.concatenate(
        [rho_row, gamma_row, delta_row, eps_row, jnp.zeros((4, 128), f32)], axis=0
    )
    partial = jnp.sum(partial, axis=1, keepdims=True)
    own = jnp.sum(jnp.where(sub8 == lane8, partial, 0.0), axis=0, keepdims=True)
    sums[...] = own

    def share_sums(device, index):
        pltpu.make_async_remote_copy(
            src_ref=sums,
            dst_ref=sums_in.at[index],
            send_sem=sum_send,
            recv_sem=sum_recv,
            device_id=device,
            device_id_type=MESH,
        ).start()

    each_other(share_sums)
    t_vec = assemble(lw, 6)
    arrived = pltpu.make_async_remote_copy(
        src_ref=sums_in,
        dst_ref=sums_in,
        send_sem=sum_send,
        recv_sem=sum_recv,
        device_id=tuple(lax.rem(me[i] + 1, counts[i]) for i in range(3)),
        device_id_type=MESH,
    )
    arrived.wait_recv()
    joined = own + jnp.sum(sums_in[...], axis=0)
    four = jnp.sum(jnp.where(sub8 == lane8, joined, 0.0), axis=1, keepdims=True)
    rho, gamma, delta, eps = (four[i : i + 1].reshape(1, 1, 1) for i in range(4))
    alpha0 = rho / gamma
    rho1 = rho - 2.0 * alpha0 * gamma + alpha0 * alpha0 * delta
    beta = rho1 / rho
    cross = gamma - alpha0 * delta
    curve = gamma - 2.0 * alpha0 * delta + alpha0 * alpha0 * eps
    curve = curve + 2.0 * beta * cross + beta * beta * gamma
    alpha1 = rho1 / curve
    along = alpha0 + alpha1 * (1.0 + beta)
    side_step = alpha0 * alpha1

    pre_ref[...] = put(
        jnp.concatenate([(along * z0[t] - side_step * w[t])[0] for t in range(4)], axis=1)
    )
    res_ref[...] = put(
        jnp.concatenate(
            [(r0[t] - along * s[t] + side_step * t_vec[t])[0] for t in range(4)], axis=1
        )
    )
    sent()
    arrived.wait_send()


def finish_kernel(adv_ref, pre_ref, res_ref, adv_out, pre_out, res_out):
    adv_out[...] = adv_ref[...]
    pre_out[...] = pre_ref[...]
    res_out[...] = res_ref[...]


def per_device(counts, velocity, inv_density, element_place):
    f32 = jnp.float32
    rows, forward, backward, square = constants()
    elements = element_place.shape[0]
    points = inv_density.shape[0]
    vmem = pl.BlockSpec(memory_space=pltpu.VMEM)
    faces = pltpu.VMEM((ROUNDS, 2, 8, 128), f32)
    faces_z = pltpu.VMEM((ROUNDS, 2, 4, 8, 128), f32)
    dma = pltpu.SemaphoreType.DMA
    others = counts[0] * counts[1] * counts[2] - 1
    shapes = (
        jax.ShapeDtypeStruct((3, elements, points), f32),
        jax.ShapeDtypeStruct((elements, points), f32),
        jax.ShapeDtypeStruct((elements, points), f32),
    )
    computed = pl.pallas_call(
        functools.partial(kernel, counts),
        out_shape=shapes,
        in_specs=[vmem, vmem, pl.BlockSpec(memory_space=pltpu.SMEM), vmem, vmem, vmem, vmem],
        out_specs=(vmem, vmem, vmem),
        scratch_shapes=[
            faces,
            faces,
            faces_z,
            pltpu.VMEM((ROUNDS, 27, 8, 128), f32),
            faces_z,
            pltpu.VMEM((1, 128), f32),
            pltpu.VMEM((others, 1, 128), f32),
            dma((11,)),
            dma((ROUNDS, 11)),
            dma,
            dma,
        ],
        compiler_params=pltpu.CompilerParams(collective_id=0, has_side_effects=True),
    )(
        velocity.transpose(0, 2, 1),
        inv_density.T,
        element_place,
        jnp.asarray(rows),
        jnp.asarray(forward),
        jnp.asarray(backward),
        jnp.asarray(square),
    )
    advected, pressure, residual = pl.pallas_call(
        finish_kernel,
        out_shape=shapes,
        in_specs=[vmem, vmem, vmem],
        out_specs=(vmem, vmem, vmem),
    )(*computed)
    return advected.transpose(0, 2, 1), pressure.T, residual.T


def solution(mesh):
    counts = tuple(mesh.shape[name] for name in AXES)
    placed = (P(None, None, AXES), P(None, AXES), P(AXES))
    return jax.shard_map(
        functools.partial(per_device, counts),
        mesh=mesh,
        in_specs=placed,
        out_specs=(P(None, None, AXES), P(None, AXES), P(None, AXES)),
        check_vma=False,
    )
```
